32 devices in a mesh: groups: 2 (over y), ep: 16 (over z, x, core).
Axes of the slice: x: 2, y: 2, z: 4, core: 2. Of those that a mesh axis runs over, the one named last changes fastest.
Arguments:
- tokens: bfloat16 [128, 7168], P(('groups', 'ep')), parts along dimension 0, may hold values from -6 to 6
- routes: int32 [128, 1], P(('groups', 'ep')), parts along dimension 0, may hold values from 0 to 1; in each aligned block of 4 rows (0 to 3, 4 to 7, ...) at most 2 rows name the same one
- router_weight: bfloat16 [7168, 2], replicated, may hold values from -0.0625 to 0.0625
- w_gate: bfloat16 [7168, 4096], P(None, 'ep'), may hold values from -0.0625 to 0.0625
- w_up: bfloat16 [7168, 4096], P(None, 'ep'), may hold values from -0.0625 to 0.0625
- w_down: bfloat16 [4096, 7168], P('ep'), may hold values from -0.125 to 0.125
- latent_pool: bfloat16 [512, 4608], P(('groups', 'ep')), parts along dimension 0, may hold values from -8 to 8
- send_order: int32 [32, 16], P(('groups', 'ep')), parts along dimension 0, may hold values from 0 to 15, each once within a row
- block_table: int32 [32, 16], P(('groups', 'ep')), parts along dimension 0, may hold values from 0 to 15, each once within a row
- seq_lens: int32 [128], P(('groups', 'ep')), parts along dimension 0, may hold values from 1 to 32
- queries: bfloat16 [128, 73728], P(('groups', 'ep')), parts along dimension 0, may hold values from -10 to 10
Outputs:
- expert_out: bfloat16 [128, 7168], P(('groups', 'ep')), parts along dimension 0
- attended: bfloat16 [128, 65536], P(('groups', 'ep')), parts along dimension 0
The draws below stay inside these ranges and needn't reach their ends.
There are 2 independent parts, one for each index of `groups`. The reference program is written for one: setup_inputs(seed, part) draws one part's arguments, and reference() takes and returns one part's arrays. A program takes and returns all parts, laid end to end along the dimension named above; an argument that names none is the same for every part. Nothing has to cross between parts.
Inputs may be any that keep to these rules, and one draw needn't show every extreme that they name: `routes`: among the 4 rows of one device no expert is named by more than 2 rows, a bound that some block reaches. `send_order`: each row is a permutation of 0 to 15. `block_table`: each row is a permutation of 0 to 15.
All inputs are finite; a program needn't handle non-finite values.
Results may differ from the reference program's by a relative error of at most 0.01.
Values may be sent and summed in bfloat16 or wider, within the bound.
No kernel may reach another device: no remote copies, remote signals or barrier semaphores. Data moves between devices by JAX's collectives and lax.ppermute only.
A program may use at most 128 MiB of HBM per device.

```python
import math
import jax
import jax.numpy as jnp
import numpy as np
from jax import lax

D = 7168
FF = 2048
LATENT_RANK = 512
ROTARY_WIDTH = 64
ATTENTION_HEADS = 128
FF_DEV = 256
TOK_DEV = 4
DEC_DEV = 4
BLOCK = 8
EXPERTS = 2
TOP = 1
CAP = 2
TOKENS = 64
MAXB = 4
DECODE_COUNT = 64
N_EP = 16


def draw_latent_pool(key, part):
    compressed_width = LATENT_RANK + ROTARY_WIDTH
    shape = (N_EP * N_EP, BLOCK, compressed_width)
    values = jnp.clip(jax.random.normal(jax.random.fold_in(key, 11), shape, jnp.float32), -6.0, 6.0)
    return values.reshape(N_EP * N_EP, BLOCK * compressed_width).astype(jnp.bfloat16)


def draw_queries(key, part):
    compressed_width = LATENT_RANK + ROTARY_WIDTH
    shape = (DEC_DEV * N_EP, ATTENTION_HEADS, compressed_width)
    values = jnp.clip(jax.random.normal(jax.random.fold_in(key, 23), shape, jnp.float32), -6.0, 6.0)
    return values.reshape(DEC_DEV * N_EP, ATTENTION_HEADS * compressed_width).astype(jnp.bfloat16)


def with_ends(drawn, own_key, low, top_value):
    longest = drawn.shape.index(max(drawn.shape))
    spots = []
    for shift in (0, 1):
        where = [jax.random.randint(jax.random.fold_in(own_key, axis), (), 0, length) for axis, length in enumerate(drawn.shape)]
        where[longest] = (where[longest] + shift) % drawn.shape[longest]
        spots.append(tuple(where))
    return drawn.at[spots[0]].set(low).at[spots[1]].set(top_value)


def block_scale(rng, shape, pieces, low, high):
    gain, own = 1.0, jax.random.fold_in(rng, 6)
    for dim, blocks in pieces:
        heights = jnp.exp(jax.random.uniform(jax.random.fold_in(own, dim), (blocks,), jnp.float32, low / len(pieces), high / len(pieces)))
        gain = gain * jnp.repeat(heights, shape[dim] // blocks).reshape([-1 if axis == dim else 1 for axis in range(len(shape))])
    return gain


def shared_out(stream_key, own, number, rows, count, top, reach, slope):
    ranking = jax.random.permutation(stream_key, count)
    packed, common = shares(count, rows * top, reach, slope, True), shares(count, rows * top, reach, slope, False)
    places = jnp.arange(count)

    def named(tallies, offset_by):
        used = int((tallies > 0).sum())
        fixed = max(1, used // 4)
        passed = fixed + (places - fixed + offset_by * (used - fixed)) % max(1, count - fixed)
        return jnp.zeros((count,), jnp.int32).at[ranking[jnp.where(places < fixed, places, passed)]].set(jnp.asarray(tallies, jnp.int32))

    tallies = jnp.where(number % 4 == 0, named(packed, number // 4), named(common, number - number // 4 - 1))
    mixed = jax.random.permutation(jax.random.fold_in(own, 3), count)
    giver, taker = mixed[0:count // 2 * 2:2], mixed[1:count // 2 * 2:2]
    slack = jnp.minimum(tallies[giver] - 1, reach - tallies[taker]) // 2
    slack = jnp.where((giver == ranking[0]) | (taker == ranking[0]) | (tallies[taker] == 0), 0, jnp.maximum(slack, 0))
    passed = jax.random.randint(jax.random.fold_in(own, 4), (count // 2,), 0, 1 << 20) % (slack + 1)
    tallies = tallies.at[giver].add(-passed).at[taker].add(passed)
    labels = jnp.searchsorted(jnp.cumsum(tallies), jnp.arange(rows * top), side="right").astype(jnp.int32)
    grid = labels.reshape(top, rows).T
    grid = grid[jax.random.permutation(jax.random.fold_in(own, 1), rows)]
    offset_by = jax.random.randint(jax.random.fold_in(own, 2), (rows, 1), 0, top)
    return jnp.take_along_axis(grid, (jnp.arange(top)[None, :] + offset_by) % top, axis=1)


def shares(number_of, total, bound, slope, full):
    weights = [(1 << 20) // math.isqrt(rank ** slope) + 1 for rank in range(1, number_of + 1)]
    largest = bound if full else min(bound, max(-(-total // number_of), total * weights[0] // sum(weights)))
    least = 1 if total - largest >= number_of - 1 else 0
    holding, rest = [largest] + [least] * (number_of - 1), total - largest - least * (number_of - 1)
    while rest > 0:
        free = [i for i in range(1, number_of) if holding[i] < largest] or [i for i in range(1, number_of) if holding[i] < bound]
        mass, remaining = sum([weights[i] for i in free]), rest
        for i in free:
            addition = min(bound - holding[i], max(1, remaining * weights[i] // mass), rest)
            holding[i] = holding[i] + addition
            rest = rest - addition
    return np.array(holding)


def noise(key, extent, spread, most, shards=(), kind=jnp.bfloat16):
    gain = block_scale(key, extent, shards, -0.22, 0.18) if shards else 1.0
    values = jax.random.normal(key, extent, jnp.float32) * spread * gain
    return jnp.minimum(jnp.maximum(values, -most), most).astype(kind)


def setup_inputs(seed: int = 0, part: int = 0) -> dict:
    keys = jax.random.split(jax.random.key(seed), 12)
    own_keys = jax.random.split(jax.random.fold_in(keys[11], part), 12)
    tokens = noise(own_keys[0], (TOKENS, D), 1.0, 6.0, ((0, 16),))
    routes_keys = jax.random.split(jax.random.fold_in(own_keys[1], 1), TOKENS // TOK_DEV)
    routes_turns = jax.random.permutation(jax.random.fold_in(own_keys[1], 3), TOKENS // TOK_DEV)
    routes = jax.vmap(lambda own, number: shared_out(jax.random.fold_in(own_keys[1], 2), own, number, TOK_DEV, EXPERTS, TOP, CAP, 2))(routes_keys, routes_turns).reshape((TOKENS, TOP))
    router_weight = noise(keys[2], (D, EXPERTS), D ** -0.5, 0.0625)
    w_gate = noise(keys[3], (D, EXPERTS * FF), D ** -0.5, 0.0625, ((1, 16),))
    w_up = noise(keys[4], (D, EXPERTS * FF), D ** -0.5, 0.0625, ((1, 16),))
    w_down = noise(keys[5], (EXPERTS * FF, D), FF ** -0.5, 0.125, ((0, 16),))
    latent_pool = draw_latent_pool(jax.random.fold_in(jax.random.fold_in(keys[11], part), 71), part)
    send_order = jax.vmap(lambda own: jax.random.permutation(own, N_EP))(jax.random.split(own_keys[7], N_EP)).reshape((N_EP, N_EP)).astype(jnp.int32)
    block_table = jax.vmap(lambda own: jax.random.permutation(own, N_EP))(jax.random.split(own_keys[8], N_EP)).reshape((N_EP, N_EP)).astype(jnp.int32)
    seq_lens = with_ends(jax.random.randint(own_keys[9], (DECODE_COUNT,), 1, MAXB * BLOCK + 1), jax.random.fold_in(own_keys[9], 1), 1, MAXB * BLOCK).astype(jnp.int32)
    queries = draw_queries(jax.random.fold_in(jax.random.fold_in(keys[11], part), 71), part)
    return dict(tokens=tokens, routes=routes, router_weight=router_weight, w_gate=w_gate, w_up=w_up, w_down=w_down, latent_pool=latent_pool, send_order=send_order, block_table=block_table, seq_lens=seq_lens, queries=queries)


route_scale = 2.5
softmax_scale = 192.0 ** -0.5


def reference(tokens, routes, router_weight, w_gate, w_up, w_down, latent_pool, send_order, block_table, seq_lens, queries):
    scores = jax.nn.sigmoid(jnp.dot(tokens, router_weight, preferred_element_type=jnp.float32))
    chosen = jnp.sum((routes[:, :, None] == jnp.arange(EXPERTS, dtype=jnp.int32)[None, None, :]).astype(jnp.float32), axis=1)
    weighted = scores * chosen
    gate_share = route_scale * weighted / jnp.sum(weighted, axis=-1, keepdims=True)
    chosen_dev = chosen.reshape(N_EP, TOK_DEV, EXPERTS)
    earlier = jnp.cumsum(chosen_dev, axis=1) - chosen_dev
    share_dev = gate_share.reshape(N_EP, TOK_DEV, EXPERTS)
    tok_dev = tokens.reshape(N_EP, TOK_DEV, D).astype(jnp.float32)
    slot_ids = jnp.arange(CAP, dtype=jnp.float32)
    shard_total = FF // FF_DEV

    def one_expert(carry_sum, expert_id):
        picked = lax.dynamic_slice_in_dim(chosen_dev, expert_id, 1, 2)[:, :, 0]
        before = lax.dynamic_slice_in_dim(earlier, expert_id, 1, 2)[:, :, 0]
        share = lax.dynamic_slice_in_dim(share_dev, expert_id, 1, 2)[:, :, 0]
        placed = ((picked[:, None, :] > 0.5) & (before[:, None, :] == slot_ids[None, :, None])).astype(jnp.float32)
        rows_e = jnp.einsum("pct,ptd->pcd", placed, tok_dev, precision=lax.Precision.HIGHEST).astype(jnp.bfloat16).reshape(N_EP * CAP, D)
        start = (expert_id * FF).astype(jnp.int32)
        gate_cols = lax.dynamic_slice_in_dim(w_gate, start, FF, 1)
        up_cols = lax.dynamic_slice_in_dim(w_up, start, FF, 1)
        down_rows = lax.dynamic_slice_in_dim(w_down, start, FF, 0)
        gate_out = jnp.dot(rows_e, gate_cols, preferred_element_type=jnp.float32)
        up_out = jnp.dot(rows_e, up_cols, preferred_element_type=jnp.float32)
        hidden_e = (jax.nn.silu(gate_out) * up_out).astype(jnp.bfloat16)
        hidden_split = hidden_e.reshape(N_EP * CAP, shard_total, FF_DEV).astype(jnp.float32)
        down_split = down_rows.reshape(shard_total, FF_DEV, D).astype(jnp.float32)
        part_e = jnp.einsum("rsf,sfd->rsd", hidden_split, down_split).astype(jnp.bfloat16)
        part_e = lax.optimization_barrier(part_e)
        y_e = jnp.sum(part_e.astype(jnp.float32), axis=1).reshape(N_EP, CAP, D)
        mixing = placed * share[:, None, :]
        carry_sum = carry_sum + jnp.einsum("pct,pcd->ptd", mixing, y_e, precision=lax.Precision.HIGHEST)
        return carry_sum, None

    start_sum = jnp.zeros((N_EP, TOK_DEV, D), jnp.float32)
    total, unused = lax.scan(one_expert, start_sum, jnp.arange(EXPERTS, dtype=jnp.int32))
    expert_out = total.reshape(TOKENS, D).astype(jnp.bfloat16)

    compressed_width = LATENT_RANK + ROTARY_WIDTH
    receiver = jnp.arange(N_EP, dtype=jnp.int32)[:, None]
    local_block = send_order[block_table, receiver]
    pool_rows = (block_table * N_EP + local_block).astype(jnp.int32)
    cached_latent_rows = jnp.take(latent_pool, pool_rows.reshape(-1), axis=0).reshape(DECODE_COUNT, MAXB * BLOCK, compressed_width)
    query_rows = queries.reshape(DECODE_COUNT, ATTENTION_HEADS, compressed_width)
    logits = jnp.einsum("shc,slc->shl", query_rows.astype(jnp.float32), cached_latent_rows.astype(jnp.float32)) * softmax_scale
    visible = jnp.arange(MAXB * BLOCK, dtype=jnp.int32)[None, None, :] < seq_lens[:, None, None]
    logits = jnp.where(visible, logits, -1e30)
    row_peak = jnp.max(logits, axis=-1, keepdims=True)
    unnormed = jnp.exp(logits - row_peak)
    routing_weight = (unnormed / jnp.sum(unnormed, axis=-1, keepdims=True)).astype(jnp.bfloat16)
    latent_states = cached_latent_rows[:, :, :LATENT_RANK]
    attended = jnp.einsum("djp,dpz->djz", routing_weight.astype(jnp.float32), latent_states.astype(jnp.float32))
    attended = attended.astype(jnp.bfloat16).reshape(DECODE_COUNT, ATTENTION_HEADS * LATENT_RANK)
    return expert_out, attended
```

```python
import functools

import jax
import jax.numpy as jnp
from jax import lax
from jax.experimental import pallas as pl
from jax.experimental.pallas import tpu as pltpu
from jax.sharding import PartitionSpec as P

LATENT_RANK = 512
ROTARY_WIDTH = 64
BLOCK = 8


route_scale = 2.5
softmax_scale = 192.0 ** (-0.5)


def vmem():
    return pl.BlockSpec(memory_space=pltpu.VMEM)


def smem():
    return pl.BlockSpec(memory_space=pltpu.SMEM)


def placements(routes_ref, mine, blocks, caps, axis):
    tok_rows, top = routes_ref.shape
    shape = (blocks * caps, 128) if axis == 0 else (tok_rows, blocks * caps)
    row = lax.broadcasted_iota(jnp.int32, shape, axis)
    expert = (row // caps) ^ mine
    slot = row % caps
    count = jnp.zeros(shape, jnp.int32)
    out = []
    for t in range(tok_rows):
        hit = expert == routes_ref[t, 0]
        for j in range(1, top):
            hit = hit | (expert == routes_ref[t, j])
        out.append(hit & (count == slot))
        count = count + hit.astype(jnp.int32)
    return out


def pack_kernel(caps, mine_ref, routes_ref, tokens_ref, *out_refs):
    blocks = len(out_refs)
    width = tokens_ref.shape[1]
    placed = placements(routes_ref, mine_ref[0], blocks, caps, 0)
    tokens = tokens_ref[...].astype(jnp.float32)
    rows = jnp.zeros((blocks * caps, width), jnp.float32)
    for t, hit in enumerate(placed):
        rows = rows + jnp.where(hit[:, :1], tokens[t : t + 1, :], 0.0)
    rows = rows.astype(jnp.bfloat16)
    for b in range(blocks):
        out_refs[b][...] = rows[b * caps : (b + 1) * caps, :]


def mix_kernel(caps, mine_ref, routes_ref, tokens_ref, centroids_ref, out_ref):
    tok_rows, top = routes_ref.shape
    experts = centroids_ref.shape[0]
    mine = mine_ref[0]
    scores = jax.nn.sigmoid(
        lax.dot_general(
            tokens_ref[...],
            centroids_ref[...],
            (((1,), (1,)), ((), ())),
            preferred_element_type=jnp.float32,
        )
    )
    expert = lax.broadcasted_iota(jnp.int32, (tok_rows, experts), 1)
    token = lax.broadcasted_iota(jnp.int32, (tok_rows, experts), 0)
    chosen = jnp.zeros((tok_rows, experts), jnp.float32)
    for t in range(tok_rows):
        for j in range(top):
            hit = (token == t) & (expert == routes_ref[t, j])
            chosen = jnp.where(hit, chosen + 1.0, chosen)
    weighted = scores * chosen
    share = route_scale * weighted / jnp.sum(weighted, axis=-1, keepdims=True)
    shape = (tok_rows, experts * caps)
    row = lax.broadcasted_iota(jnp.int32, shape, 1)
    row_expert = (row // caps) ^ mine
    row_share = jnp.zeros(shape, jnp.float32)
    for e in range(experts):
        row_share = jnp.where(row_expert == e, share[:, e : e + 1], row_share)
    placed = placements(routes_ref, mine, experts, caps, 1)
    row_token = lax.broadcasted_iota(jnp.int32, shape, 0)
    mixing = jnp.zeros(shape, jnp.float32)
    for t, hit in enumerate(placed):
        mixing = jnp.where((row_token == t) & hit, row_share, mixing)
    out_ref[...] = mixing


def ffn_kernel(
    chunks, near_ref, far_ref, gate_hbm, up_hbm, down_hbm, keep_ref, send_ref, gate, up, down, sems
):
    width, units = gate.shape
    step = width // chunks
    half = near_ref.shape[0]

    def copies(i):
        part = pl.ds(i * step, step)
        return (
            pltpu.make_async_copy(gate_hbm.at[part, :], gate.at[part, :], sems.at[0, i]),
            pltpu.make_async_copy(up_hbm.at[part, :], up.at[part, :], sems.at[1, i]),
        )

    def down_copy(i):
        part = pl.ds(i * step, step)
        return pltpu.make_async_copy(down_hbm.at[:, part], down.at[:, part], sems.at[2, i])

    for i in range(chunks):
        for copy in copies(i):
            copy.start()
    for i in range(chunks):
        down_copy(i).start()
    gate_sum = jnp.zeros((2 * half, units), jnp.float32)
    up_sum = jnp.zeros((2 * half, units), jnp.float32)
    for i in range(chunks):
        part = pl.ds(i * step, step)
        rows = jnp.concatenate([near_ref[:, part], far_ref[:, part]], axis=0)
        gate_copy, up_copy = copies(i)
        gate_copy.wait()
        gate_sum += jnp.dot(rows, gate[part, :], preferred_element_type=jnp.float32)
        up_copy.wait()
        up_sum += jnp.dot(rows, up[part, :], preferred_element_type=jnp.float32)
    hidden = (gate_sum * jax.nn.sigmoid(gate_sum) * up_sum).astype(jnp.bfloat16)
    for i in range(chunks):
        part = pl.ds(i * step, step)
        down_copy(i).wait()
        result = jnp.dot(hidden, down[:, part], preferred_element_type=jnp.float32)
        result = result.astype(jnp.bfloat16)
        keep_ref[:, part] = result[:half, :]
        send_ref[:, part] = result[half:, :]


def body(
    tokens,
    routes,
    router_weight,
    w_gate,
    w_up,
    w_down,
    latent_pool,
    send_order,
    block_table,
    seq_lens,
    queries,
):
    device_count = lax.axis_size("ep")
    tok_rows, width = tokens.shape
    experts = router_weight.shape[1]
    top_count = routes.shape[1]
    shard_count = device_count // experts
    capacity = tok_rows * top_count // experts + tok_rows * top_count // (4 * experts)
    mine = (lax.axis_index("ep") // shard_count).astype(jnp.int32).reshape(1)

    def exchange(value, mask):
        return lax.ppermute(value, "ep", [(i, i ^ mask) for i in range(device_count)])

    packed = pl.pallas_call(
        functools.partial(pack_kernel, capacity),
        out_shape=[jax.ShapeDtypeStruct((capacity, width), jnp.bfloat16)] * experts,
        in_specs=[smem(), smem(), vmem()],
        out_specs=[vmem()] * experts,
    )(mine, routes, tokens)
    crossed = [exchange(packed[b], b * shard_count) for b in range(1, experts)]
    rows = jnp.concatenate([packed[0]] + crossed, axis=0)
    near = jnp.concatenate([rows] + [exchange(rows, m) for m in range(2, shard_count, 2)], axis=0)
    far = exchange(near, 1)

    compressed_width = LATENT_RANK + ROTARY_WIDTH
    block_ids = jnp.arange(device_count, dtype=jnp.int32)
    picks = (send_order[0][:, None] == block_ids[None, :]).astype(jnp.bfloat16)
    outgoing_blocks = jnp.dot(picks, latent_pool, preferred_element_type=jnp.float32).astype(jnp.bfloat16)
    arrived = lax.all_to_all(outgoing_blocks, "ep", split_axis=0, concat_axis=0, tiled=True)

    half = near.shape[0]
    units = w_gate.shape[1]
    chunks = 7
    keep, send = pl.pallas_call(
        functools.partial(ffn_kernel, chunks),
        out_shape=[jax.ShapeDtypeStruct((half, width), jnp.bfloat16)] * 2,
        in_specs=[vmem(), vmem()] + [pl.BlockSpec(memory_space=pltpu.HBM)] * 3,
        out_specs=[vmem(), vmem()],
        scratch_shapes=[
            pltpu.VMEM((width, units), jnp.bfloat16),
            pltpu.VMEM((width, units), jnp.bfloat16),
            pltpu.VMEM((units, width), jnp.bfloat16),
            pltpu.SemaphoreType.DMA((3, chunks)),
        ],
        compiler_params=pltpu.CompilerParams(vmem_limit_bytes=24 * 1024 * 1024),
        cost_estimate=pl.CostEstimate(
            flops=12 * half * width * units, bytes_accessed=6 * width * units, transcendentals=0
        ),
    )(near, far, w_gate, w_up, w_down)

    paired = keep.astype(jnp.float32) + exchange(send, 1).astype(jnp.float32)
    slots = experts * capacity
    paired = paired.reshape(shard_count // 2, slots, width)
    total = paired[0]
    for k in range(1, shard_count // 2):
        total = total + exchange(paired[k].astype(jnp.bfloat16), 2 * k).astype(jnp.float32)
    total = total.reshape(experts, capacity, width)
    summed = [total[0]] + [
        exchange(total[b].astype(jnp.bfloat16), b * shard_count).astype(jnp.float32)
        for b in range(1, experts)
    ]
    mixing = pl.pallas_call(
        functools.partial(mix_kernel, capacity),
        out_shape=jax.ShapeDtypeStruct((tok_rows, slots), jnp.float32),
        in_specs=[smem(), smem(), vmem(), vmem()],
        out_specs=vmem(),
    )(mine, routes, tokens, router_weight.T)
    expert_out = jnp.zeros((tok_rows, width), jnp.float32)
    for b in range(experts):
        for c in range(capacity):
            r = b * capacity + c
            expert_out = expert_out + mixing[:, r : r + 1] * summed[b][c : c + 1, :]
    expert_out = expert_out.astype(jnp.bfloat16)

    sequence_total = seq_lens.shape[0]
    span_length = device_count // sequence_total * BLOCK
    cached_latent_rows = jnp.take(arrived, block_table[0], axis=0).reshape(
        sequence_total, span_length, compressed_width
    )
    attention_head_count = queries.shape[1] // compressed_width
    query_rows = queries.reshape(sequence_total, attention_head_count, compressed_width)
    logits = (
        jnp.einsum(
            "shc,slc->shl", query_rows, cached_latent_rows, preferred_element_type=jnp.float32
        )
        * softmax_scale
    )
    visible = jnp.arange(span_length, dtype=jnp.int32)[None, None, :] < seq_lens[:, None, None]
    logits = jnp.where(visible, logits, -1e30)
    row_peak = jnp.max(logits, axis=-1, keepdims=True)
    unnormed = jnp.exp(logits - row_peak)
    routing_weight = (unnormed / jnp.sum(unnormed, axis=-1, keepdims=True)).astype(jnp.bfloat16)
    attended = jnp.einsum(
        "djp,dpz->djz",
        routing_weight,
        cached_latent_rows[:, :, :LATENT_RANK],
        preferred_element_type=jnp.float32,
    )
    attended = attended.astype(jnp.bfloat16).reshape(
        sequence_total, attention_head_count * LATENT_RANK
    )
    return (expert_out, attended)


def solution(mesh):
    return jax.shard_map(
        body,
        mesh=mesh,
        in_specs=(
            P(("groups", "ep"), None),
            P(("groups", "ep"), None),
            P(),
            P(None, "ep"),
            P(None, "ep"),
            P("ep", None),
            P(("groups", "ep"), None),
            P(("groups", "ep"), None),
            P(("groups", "ep"), None),
            P(("groups", "ep")),
            P(("groups", "ep"), None),
        ),
        out_specs=(P(("groups", "ep"), None), P(("groups", "ep"), None)),
        check_vma=False,
    )
```

```python
import functools

import jax
import jax.numpy as jnp
from jax import lax
from jax.experimental import pallas as pl
from jax.experimental.pallas import tpu as pltpu
from jax.sharding import PartitionSpec as P


LATENT_RANK = 512
ROTARY_WIDTH = 64
BLOCK = 8


route_scale = 2.5
softmax_scale = 192.0 ** (-0.5)


def vmem():
    return pl.BlockSpec(memory_space=pltpu.VMEM)


def smem():
    return pl.BlockSpec(memory_space=pltpu.SMEM)


def in_hbm(value):
    return pltpu.with_memory_space_constraint(value, pltpu.HBM)


def placements(routes_ref, mine, blocks, caps, axis):
    top, tok_rows = routes_ref.shape
    shape = (blocks * caps, 128) if axis == 0 else (tok_rows, blocks * caps)
    row = lax.broadcasted_iota(jnp.int32, shape, axis)
    expert = (row // caps) ^ mine
    slot = row % caps
    count = jnp.zeros(shape, jnp.int32)
    out = []
    for t in range(tok_rows):
        hit = expert == routes_ref[0, t]
        for j in range(1, top):
            hit = hit | (expert == routes_ref[j, t])
        out.append(hit & (count == slot))
        count = count + hit.astype(jnp.int32)
    return out


def pack_kernel(caps, mine_ref, routes_ref, tokens_ref, *out_refs):
    blocks = len(out_refs)
    width = tokens_ref.shape[1]
    placed = placements(routes_ref, mine_ref[0], blocks, caps, 0)
    tokens = tokens_ref[...].astype(jnp.float32)
    rows = jnp.zeros((blocks * caps, width), jnp.float32)
    for t, hit in enumerate(placed):
        rows = rows + jnp.where(hit[:, :1], tokens[t : t + 1, :], 0.0)
    rows = rows.astype(jnp.bfloat16)
    for b in range(blocks):
        out_refs[b][...] = rows[b * caps : (b + 1) * caps, :]


def mix_kernel(caps, mine_ref, routes_ref, tokens_ref, centroids_ref, out_ref):
    top, tok_rows = routes_ref.shape
    experts = centroids_ref.shape[0]
    mine = mine_ref[0]
    scores = jax.nn.sigmoid(
        lax.dot_general(
            tokens_ref[...],
            centroids_ref[...],
            (((1,), (1,)), ((), ())),
            preferred_element_type=jnp.float32,
        )
    )
    expert = lax.broadcasted_iota(jnp.int32, (tok_rows, experts), 1)
    token = lax.broadcasted_iota(jnp.int32, (tok_rows, experts), 0)
    chosen = jnp.zeros((tok_rows, experts), jnp.float32)
    for t in range(tok_rows):
        for j in range(top):
            hit = (token == t) & (expert == routes_ref[j, t])
            chosen = jnp.where(hit, chosen + 1.0, chosen)
    weighted = scores * chosen
    share = route_scale * weighted / jnp.sum(weighted, axis=-1, keepdims=True)
    shape = (tok_rows, experts * caps)
    row = lax.broadcasted_iota(jnp.int32, shape, 1)
    row_expert = (row // caps) ^ mine
    row_share = jnp.zeros(shape, jnp.float32)
    for e in range(experts):
        row_share = jnp.where(row_expert == e, share[:, e : e + 1], row_share)
    placed = placements(routes_ref, mine, experts, caps, 1)
    row_token = lax.broadcasted_iota(jnp.int32, shape, 0)
    mixing = jnp.zeros(shape, jnp.float32)
    for t, hit in enumerate(placed):
        mixing = jnp.where((row_token == t) & hit, row_share, mixing)
    out_ref[...] = mixing


def outgoing_kernel(order_ref, pool_ref, out_ref):
    count, _, half = out_ref.shape
    blocks = pool_ref.shape[0]
    row = lax.broadcasted_iota(jnp.int32, (2 * count, blocks), 0)
    block = lax.broadcasted_iota(jnp.int32, (2 * count, blocks), 1)
    wanted = jnp.zeros((2 * count, blocks), jnp.int32)
    for d in range(count):
        wanted = jnp.where(row // 2 == d, order_ref[0, d], wanted)
    hit = block == wanted
    result = jnp.zeros((2 * count, half), jnp.float32)
    for r in range(2):
        picks = jnp.where(hit & (row % 2 == r), 1.0, 0.0).astype(jnp.bfloat16)
        result = result + jnp.dot(
            picks, pool_ref[:, r * half : (r + 1) * half], preferred_element_type=jnp.float32
        )
    result = result.astype(jnp.bfloat16)
    for d in range(count):
        out_ref[d] = result[2 * d : 2 * d + 2, :]


def attention_kernel(table_ref, lens_ref, queries_ref, arrived_ref, out_ref):
    sequences, _, entries = queries_ref.shape
    rows = arrived_ref.shape[0]
    per_row = BLOCK // 2
    per_sequence = rows // 2 // sequences
    arrived = arrived_ref[...]
    cache = jnp.concatenate(
        [arrived[:, i * entries : (i + 1) * entries] for i in range(per_row)], axis=0
    )
    keys = cache.shape[0]
    key = lax.broadcasted_iota(jnp.int32, (1, keys), 1)
    source = (key % rows) // 2
    token = (key % 2) * per_row + key // rows
    for s in range(sequences):
        position = jnp.full((1, keys), per_sequence * BLOCK, jnp.int32)
        for b in range(per_sequence):
            position = jnp.where(
                source == table_ref[0, s * per_sequence + b], b * BLOCK + token, position
            )
        visible = position < lens_ref[s]
        logits = lax.dot_general(
            queries_ref[s], cache, (((1,), (1,)), ((), ())), preferred_element_type=jnp.float32
        )
        logits = jnp.where(visible, logits * softmax_scale, -1e30)
        peak = jnp.max(logits, axis=-1, keepdims=True)
        unnormed = jnp.exp(logits - peak)
        unnormed = jnp.where(visible, unnormed, 0.0)
        weights = (unnormed / jnp.sum(unnormed, axis=-1, keepdims=True)).astype(jnp.bfloat16)
        out_ref[s] = jnp.dot(
            weights, cache[:, :LATENT_RANK], preferred_element_type=jnp.float32
        ).astype(jnp.bfloat16)


def ffn_kernel(
    chunks, near_ref, far_ref, gate_hbm, up_hbm, down_hbm, keep_ref, send_ref, gate, up, down, sems
):
    width, units = gate.shape
    step = width // chunks
    half = near_ref.shape[0]

    def copies(i):
        part = pl.ds(i * step, step)
        return (
            pltpu.make_async_copy(gate_hbm.at[part, :], gate.at[part, :], sems.at[0, i]),
            pltpu.make_async_copy(up_hbm.at[part, :], up.at[part, :], sems.at[1, i]),
        )

    def down_copy(i):
        part = pl.ds(i * step, step)
        return pltpu.make_async_copy(down_hbm.at[:, part], down.at[:, part], sems.at[2, i])

    for i in range(chunks):
        for copy in copies(i):
            copy.start()
    for i in range(chunks):
        down_copy(i).start()
    gate_sum = jnp.zeros((2 * half, units), jnp.float32)
    up_sum = jnp.zeros((2 * half, units), jnp.float32)
    for i in range(chunks):
        part = pl.ds(i * step, step)
        rows = jnp.concatenate([near_ref[:, part], far_ref[:, part]], axis=0)
        gate_copy, up_copy = copies(i)
        gate_copy.wait()
        gate_sum += jnp.dot(rows, gate[part, :], preferred_element_type=jnp.float32)
        up_copy.wait()
        up_sum += jnp.dot(rows, up[part, :], preferred_element_type=jnp.float32)
    hidden = (gate_sum * jax.nn.sigmoid(gate_sum) * up_sum).astype(jnp.bfloat16)
    for i in range(chunks):
        part = pl.ds(i * step, step)
        down_copy(i).wait()
        result = jnp.dot(hidden, down[:, part], preferred_element_type=jnp.float32)
        result = result.astype(jnp.bfloat16)
        keep_ref[:, part] = result[:half, :]
        send_ref[:, part] = result[half:, :]


def layer(
    tokens,
    routes,
    router_weight,
    w_gate,
    w_up,
    w_down,
    latent_pool,
    send_order,
    block_table,
    seq_lens,
    queries,
):
    device_count = lax.axis_size("ep")
    tok_rows, width = tokens.shape
    experts = router_weight.shape[1]
    top_count = routes.shape[1]
    shard_count = device_count // experts
    capacity = tok_rows * top_count // experts + tok_rows * top_count // (4 * experts)
    mine = (lax.axis_index("ep") // shard_count).astype(jnp.int32).reshape(1)

    def exchange(value, mask):
        return lax.ppermute(value, "ep", [(i, i ^ mask) for i in range(device_count)])

    def kernel(body, **options):
        def call(*operands):
            return pl.pallas_call(body, **options)(*operands)

        return call

    small = pltpu.CompilerParams(vmem_limit_bytes=8 * 1024 * 1024)
    routes = routes.T

    packed = kernel(
        functools.partial(pack_kernel, capacity),
        out_shape=[jax.ShapeDtypeStruct((capacity, width), jnp.bfloat16)] * experts,
        in_specs=[smem(), smem(), vmem()],
        out_specs=[vmem()] * experts,
        compiler_params=small,
    )(mine, in_hbm(routes), in_hbm(tokens))
    crossed = [exchange(packed[b], b * shard_count) for b in range(1, experts)]
    rows = jnp.concatenate([packed[0]] + crossed, axis=0)
    spread = [exchange(rows, m) for m in range(2, shard_count, 2)]
    near = jnp.concatenate([rows] + spread, axis=0)
    far = exchange(near, 1)

    compressed_width = LATENT_RANK + ROTARY_WIDTH
    half_block = latent_pool.shape[1] // 2
    outgoing = kernel(
        outgoing_kernel,
        out_shape=jax.ShapeDtypeStruct((device_count, 2, half_block), jnp.bfloat16),
        in_specs=[smem(), vmem()],
        out_specs=vmem(),
        compiler_params=small,
    )(in_hbm(send_order), in_hbm(latent_pool))
    arrived = lax.all_to_all(outgoing, "ep", split_axis=0, concat_axis=0, tiled=True)

    half = near.shape[0]
    units = w_gate.shape[1]
    chunks = 7
    keep, send = kernel(
        functools.partial(ffn_kernel, chunks),
        out_shape=[jax.ShapeDtypeStruct((half, width), jnp.bfloat16)] * 2,
        in_specs=[vmem(), vmem()] + [pl.BlockSpec(memory_space=pl.ANY)] * 3,
        out_specs=[vmem(), vmem()],
        scratch_shapes=[
            pltpu.VMEM((width, units), jnp.bfloat16),
            pltpu.VMEM((width, units), jnp.bfloat16),
            pltpu.VMEM((units, width), jnp.bfloat16),
            pltpu.SemaphoreType.DMA((3, chunks)),
        ],
        compiler_params=pltpu.CompilerParams(vmem_limit_bytes=54000000),
        cost_estimate=pl.CostEstimate(
            flops=12 * half * width * units, bytes_accessed=6 * width * units, transcendentals=0
        ),
    )(near, far, w_gate, w_up, w_down)

    paired = keep.astype(jnp.float32) + exchange(send, 1).astype(jnp.float32)
    slots = experts * capacity
    paired = paired.reshape(shard_count // 2, slots, width)
    total = paired[0]
    for k in range(1, shard_count // 2):
        total = total + exchange(paired[k].astype(jnp.bfloat16), 2 * k).astype(jnp.float32)
    total = total.reshape(experts, capacity, width)
    summed = [total[0]] + [
        exchange(total[b].astype(jnp.bfloat16), b * shard_count).astype(jnp.float32)
        for b in range(1, experts)
    ]
    mixing = kernel(
        functools.partial(mix_kernel, capacity),
        out_shape=jax.ShapeDtypeStruct((tok_rows, slots), jnp.float32),
        in_specs=[smem(), smem(), vmem(), vmem()],
        out_specs=vmem(),
        compiler_params=small,
    )(mine, in_hbm(routes), in_hbm(tokens), in_hbm(router_weight.T))
    expert_out = jnp.zeros((tok_rows, width), jnp.float32)
    for b in range(experts):
        for c in range(capacity):
            r = b * capacity + c
            expert_out = expert_out + mixing[:, r : r + 1] * summed[b][c : c + 1, :]
    expert_out = expert_out.astype(jnp.bfloat16)

    sequence_total = seq_lens.shape[0]
    attention_head_count = queries.shape[1] // compressed_width
    query_rows = queries.reshape(sequence_total, attention_head_count, compressed_width)
    attended = kernel(
        attention_kernel,
        out_shape=jax.ShapeDtypeStruct(
            (sequence_total, attention_head_count, LATENT_RANK), jnp.bfloat16
        ),
        in_specs=[smem(), smem(), vmem(), vmem()],
        out_specs=vmem(),
        compiler_params=pltpu.CompilerParams(vmem_limit_bytes=32 * 1024 * 1024),
    )(block_table, seq_lens, query_rows, arrived.reshape(2 * device_count, half_block))
    attended = attended.reshape(sequence_total, attention_head_count * LATENT_RANK)
    return (expert_out, attended)


def solution(mesh):
    return jax.shard_map(
        layer,
        mesh=mesh,
        in_specs=(
            P(("groups", "ep"), None),
            P(("groups", "ep"), None),
            P(),
            P(None, "ep"),
            P(None, "ep"),
            P("ep", None),
            P(("groups", "ep"), None),
            P(("groups", "ep"), None),
            P(("groups", "ep"), None),
            P(("groups", "ep")),
            P(("groups", "ep"), None),
        ),
        out_specs=(P(("groups", "ep"), None), P(("groups", "ep"), None)),
        check_vma=False,
    )
```

```python
import functools

import jax
import jax.numpy as jnp
from jax import lax
from jax.experimental import pallas as pl
from jax.experimental.pallas import tpu as pltpu
from jax.sharding import PartitionSpec as P


LATENT_RANK = 512
ROTARY_WIDTH = 64
BLOCK = 8


route_scale = 2.5
softmax_scale = 192.0 ** (-0.5)


def vmem():
    return pl.BlockSpec(memory_space=pltpu.VMEM)


def smem():
    return pl.BlockSpec(memory_space=pltpu.SMEM)


def in_hbm(value):
    return pltpu.with_memory_space_constraint(value, pltpu.HBM)


def placements(routes_ref, mine, blocks, caps, axis):
    top, tok_rows = routes_ref.shape
    shape = (blocks * caps, 128) if axis == 0 else (tok_rows, blocks * caps)
    row = lax.broadcasted_iota(jnp.int32, shape, axis)
    expert = (row // caps) ^ mine
    slot = row % caps
    count = jnp.zeros(shape, jnp.int32)
    out = []
    for t in range(tok_rows):
        hit = expert == routes_ref[0, t]
        for j in range(1, top):
            hit = hit | (expert == routes_ref[j, t])
        out.append(hit & (count == slot))
        count = count + hit.astype(jnp.int32)
    return out


def pack_kernel(caps, mine_ref, routes_ref, tokens_ref, *out_refs):
    blocks = len(out_refs)
    width = tokens_ref.shape[1]
    placed = placements(routes_ref, mine_ref[0], blocks, caps, 0)
    tokens = tokens_ref[...].astype(jnp.float32)
    rows = jnp.zeros((blocks * caps, width), jnp.float32)
    for t, hit in enumerate(placed):
        rows = rows + jnp.where(hit[:, :1], tokens[t : t + 1, :], 0.0)
    rows = rows.astype(jnp.bfloat16)
    for b in range(blocks):
        out_refs[b][...] = rows[b * caps : (b + 1) * caps, :]


def mix_kernel(caps, mine_ref, routes_ref, tokens_ref, centroids_ref, out_ref):
    top, tok_rows = routes_ref.shape
    experts = centroids_ref.shape[0]
    mine = mine_ref[0]
    scores = jax.nn.sigmoid(
        lax.dot_general(
            tokens_ref[...],
            centroids_ref[...],
            (((1,), (1,)), ((), ())),
            preferred_element_type=jnp.float32,
        )
    )
    expert = lax.broadcasted_iota(jnp.int32, (tok_rows, experts), 1)
    token = lax.broadcasted_iota(jnp.int32, (tok_rows, experts), 0)
    chosen = jnp.zeros((tok_rows, experts), jnp.float32)
    for t in range(tok_rows):
        for j in range(top):
            hit = (token == t) & (expert == routes_ref[j, t])
            chosen = jnp.where(hit, chosen + 1.0, chosen)
    weighted = scores * chosen
    share = route_scale * weighted / jnp.sum(weighted, axis=-1, keepdims=True)
    shape = (tok_rows, experts * caps)
    row = lax.broadcasted_iota(jnp.int32, shape, 1)
    row_expert = (row // caps) ^ mine
    row_share = jnp.zeros(shape, jnp.float32)
    for e in range(experts):
        row_share = jnp.where(row_expert == e, share[:, e : e + 1], row_share)
    placed = placements(routes_ref, mine, experts, caps, 1)
    row_token = lax.broadcasted_iota(jnp.int32, shape, 0)
    mixing = jnp.zeros(shape, jnp.float32)
    for t, hit in enumerate(placed):
        mixing = jnp.where((row_token == t) & hit, row_share, mixing)
    out_ref[...] = mixing


def outgoing_kernel(shards, me_ref, order_ref, pool_ref, *out_refs):
    rows = out_refs[0].shape[0]
    blocks = pool_ref.shape[0]
    total = rows * len(out_refs)
    row = lax.broadcasted_iota(jnp.int32, (total, blocks), 0)
    block = lax.broadcasted_iota(jnp.int32, (total, blocks), 1)
    wanted = jnp.zeros((total, blocks), jnp.int32)
    for i in range(total):
        target = shards * (i % rows // 2) + 2 * (i // rows) + i % 2
        wanted = jnp.where(row == i, order_ref[0, me_ref[0] ^ target], wanted)
    picks = jnp.where(block == wanted, 1.0, 0.0).astype(jnp.bfloat16)
    result = jnp.dot(picks, pool_ref[...], preferred_element_type=jnp.float32)
    for m, out_ref in enumerate(out_refs):
        out_ref[...] = result[m * rows : (m + 1) * rows, :].astype(jnp.bfloat16)


def join_kernel(groups, *refs):
    row_refs, rest = refs[:groups], refs[groups:]
    block_refs, out_refs = rest[: len(rest) // 2], rest[len(rest) // 2 :]
    caps, width = row_refs[0].shape
    for block_ref, out_ref in zip(block_refs, out_refs):
        for b, row_ref in enumerate(row_refs):
            out_ref[b * caps : (b + 1) * caps, :width] = row_ref[...]
        out_ref[:, width:] = block_ref[...]


def leaving_kernel(shift, *refs):
    groups = refs[0].shape[0] // 2
    for b, out_ref in enumerate(refs[len(refs) - groups + 1 :], 1):
        for m, in_ref in enumerate(refs[: len(refs) - groups + 1]):
            out_ref[2 * m : 2 * m + 2, :] = in_ref[2 * b : 2 * b + 2, shift:]


def attention_kernel(
    groups, shards, shift, me_ref, table_ref, lens_ref, queries_ref, *refs
):
    *arrived_refs, out_ref, arrived = refs
    sequences, _, entries = queries_ref.shape
    pairs = shards // 2
    side = groups * shards
    for a in range(2):
        near_refs = arrived_refs[a * pairs : (a + 1) * pairs]
        far_refs = arrived_refs[2 * pairs + a * (groups - 1) : 2 * pairs + (a + 1) * (groups - 1)]
        for m, near_ref in enumerate(near_refs):
            arrived[a * side + 2 * m : a * side + 2 * m + 2, :] = near_ref[:2, shift:]
        for b, far_ref in enumerate(far_refs, 1):
            start = a * side + b * shards
            arrived[start : start + shards, :] = far_ref[...]
    count = side
    half = count // 2
    row = lax.broadcasted_iota(jnp.int32, (count, 2 * count), 0)
    column = lax.broadcasted_iota(jnp.int32, (count, 2 * count), 1)
    picks = jnp.where(column == 2 * row + row // half, 1.0, 0.0).astype(jnp.bfloat16)
    blocks = jnp.dot(picks, arrived[...], preferred_element_type=jnp.float32).astype(jnp.bfloat16)
    cache = jnp.concatenate(
        [blocks[:, i * entries : (i + 1) * entries] for i in range(BLOCK)], axis=0
    )
    keys = cache.shape[0]
    key = lax.broadcasted_iota(jnp.int32, (1, keys), 1)
    token = key // count
    place = key % count
    source = me_ref[0] ^ (
        place // half + 2 * (place % pairs) + shards * (place % half // pairs)
    )
    per_sequence = count // sequences
    for s in range(sequences):
        position = jnp.full((1, keys), per_sequence * BLOCK, jnp.int32)
        for b in range(per_sequence):
            position = jnp.where(
                source == table_ref[0, s * per_sequence + b], b * BLOCK + token, position
            )
        visible = position < lens_ref[s]
        logits = lax.dot_general(
            queries_ref[s], cache, (((1,), (1,)), ((), ())), preferred_element_type=jnp.float32
        )
        logits = jnp.where(visible, logits * softmax_scale, -1e30)
        peak = jnp.max(logits, axis=-1, keepdims=True)
        unnormed = jnp.exp(logits - peak)
        unnormed = jnp.where(visible, unnormed, 0.0)
        weights = (unnormed / jnp.sum(unnormed, axis=-1, keepdims=True)).astype(jnp.bfloat16)
        out_ref[s] = jnp.dot(
            weights, cache[:, :LATENT_RANK], preferred_element_type=jnp.float32
        ).astype(jnp.bfloat16)


def ffn_kernel(chunks, gate_ref, up_ref, down_ref, *refs):
    *row_refs, keep_ref, send_ref, rows = refs
    width, units = gate_ref.shape
    step = width // chunks
    half = keep_ref.shape[0]
    height = row_refs[0].shape[0]
    for i, row_ref in enumerate(row_refs):
        rows[i * height : (i + 1) * height, :] = row_ref[:, :width]
    gate_sum = jnp.zeros((2 * half, units), jnp.float32)
    up_sum = jnp.zeros((2 * half, units), jnp.float32)
    for i in range(chunks):
        part = pl.ds(i * step, step)
        gate_sum += jnp.dot(rows[:, part], gate_ref[part, :], preferred_element_type=jnp.float32)
        up_sum += jnp.dot(rows[:, part], up_ref[part, :], preferred_element_type=jnp.float32)
    hidden = (gate_sum * jax.nn.sigmoid(gate_sum) * up_sum).astype(jnp.bfloat16)
    for i in range(chunks):
        part = pl.ds(i * step, step)
        result = jnp.dot(hidden, down_ref[:, part], preferred_element_type=jnp.float32)
        result = result.astype(jnp.bfloat16)
        keep_ref[:, part] = result[:half, :]
        send_ref[:, part] = result[half:, :]


def layer(
    tokens,
    routes,
    router_weight,
    w_gate,
    w_up,
    w_down,
    latent_pool,
    send_order,
    block_table,
    seq_lens,
    queries,
):
    device_count = lax.axis_size("ep")
    tok_rows, width = tokens.shape
    experts = router_weight.shape[1]
    top_count = routes.shape[1]
    shard_count = device_count // experts
    capacity = tok_rows * top_count // experts + tok_rows * top_count // (4 * experts)
    me = lax.axis_index("ep").astype(jnp.int32).reshape(1)
    mine = me // shard_count

    def exchange(value, mask):
        return lax.ppermute(value, "ep", [(i, i ^ mask) for i in range(device_count)])

    def kernel(body, **options):
        def call(*operands):
            return pl.pallas_call(body, **options)(*operands)

        return call

    small = pltpu.CompilerParams(vmem_limit_bytes=8 * 1024 * 1024)
    routes = routes.T

    packed = kernel(
        functools.partial(pack_kernel, capacity),
        out_shape=[jax.ShapeDtypeStruct((capacity, width), jnp.bfloat16)] * experts,
        in_specs=[smem(), smem(), vmem()],
        out_specs=[vmem()] * experts,
        compiler_params=small,
    )(mine, in_hbm(routes), in_hbm(tokens))
    crossed = [exchange(packed[b], b * shard_count) for b in range(1, experts)]
    slots = experts * capacity
    assert capacity == 2

    compressed_width = LATENT_RANK + ROTARY_WIDTH
    block_width = latent_pool.shape[1]
    pairs = shard_count // 2
    outgoing = kernel(
        functools.partial(outgoing_kernel, shard_count),
        out_shape=[jax.ShapeDtypeStruct((2 * experts, block_width), jnp.bfloat16)] * pairs,
        in_specs=[smem(), smem(), vmem()],
        out_specs=[vmem()] * pairs,
        compiler_params=small,
    )(me, in_hbm(send_order), in_hbm(latent_pool))
    joined = kernel(
        functools.partial(join_kernel, experts),
        cost_estimate=pl.CostEstimate(
            flops=8 * 10**9, bytes_accessed=8 * 10**7, transcendentals=0
        ),
        out_shape=[jax.ShapeDtypeStruct((slots, width + block_width), jnp.bfloat16)] * pairs,
        in_specs=[vmem()] * (experts + pairs),
        out_specs=[vmem()] * pairs,
        compiler_params=small,
    )(packed[0], *crossed, *outgoing)
    near = [joined[0]] + [exchange(joined[m], 2 * m) for m in range(1, pairs)]
    far = [exchange(piece, 1) for piece in near]
    leaving = kernel(
        functools.partial(leaving_kernel, width),
        out_shape=[jax.ShapeDtypeStruct((shard_count, block_width), jnp.bfloat16)]
        * (experts - 1),
        in_specs=[vmem()] * pairs,
        out_specs=[vmem()] * (experts - 1),
        compiler_params=small,
    )(*near)
    entered = [exchange(leaving[b - 1], b * shard_count) for b in range(1, experts)]
    arrived = near + far + entered + [exchange(piece, 1) for piece in entered]

    half = slots * shard_count // 2
    units = w_gate.shape[1]
    chunks = 7
    keep, send = kernel(
        functools.partial(ffn_kernel, chunks),
        out_shape=[jax.ShapeDtypeStruct((half, width), jnp.bfloat16)] * 2,
        in_specs=[vmem()] * (3 + shard_count),
        out_specs=[vmem(), vmem()],
        scratch_shapes=[pltpu.VMEM((2 * half, width), jnp.bfloat16)],
        compiler_params=pltpu.CompilerParams(vmem_limit_bytes=16 * 1024 * 1024),
        cost_estimate=pl.CostEstimate(
            flops=12 * half * width * units, bytes_accessed=6 * width * units, transcendentals=0
        ),
    )(w_gate, w_up, w_down, *near, *far)

    paired = keep.astype(jnp.float32) + exchange(send, 1).astype(jnp.float32)
    paired = paired.reshape(shard_count // 2, slots, width)
    total = paired[0]
    for k in range(1, shard_count // 2):
        total = total + exchange(paired[k].astype(jnp.bfloat16), 2 * k).astype(jnp.float32)
    total = total.reshape(experts, capacity, width)
    summed = [total[0]] + [
        exchange(total[b].astype(jnp.bfloat16), b * shard_count).astype(jnp.float32)
        for b in range(1, experts)
    ]
    mixing = kernel(
        functools.partial(mix_kernel, capacity),
        out_shape=jax.ShapeDtypeStruct((tok_rows, slots), jnp.float32),
        in_specs=[smem(), smem(), vmem(), vmem()],
        out_specs=vmem(),
        compiler_params=small,
    )(mine, in_hbm(routes), in_hbm(tokens), in_hbm(router_weight.T))
    expert_out = jnp.zeros((tok_rows, width), jnp.float32)
    for b in range(experts):
        for c in range(capacity):
            r = b * capacity + c
            expert_out = expert_out + mixing[:, r : r + 1] * summed[b][c : c + 1, :]
    expert_out = expert_out.astype(jnp.bfloat16)

    sequence_total = seq_lens.shape[0]
    attention_head_count = queries.shape[1] // compressed_width
    query_rows = queries.reshape(sequence_total, attention_head_count, compressed_width)
    attended = kernel(
        functools.partial(attention_kernel, experts, shard_count, width),
        out_shape=jax.ShapeDtypeStruct(
            (sequence_total, attention_head_count, LATENT_RANK), jnp.bfloat16
        ),
        in_specs=[smem()] * 3 + [vmem()] * (1 + len(arrived)),
        out_specs=vmem(),
        scratch_shapes=[pltpu.VMEM((2 * device_count, block_width), jnp.bfloat16)],
        compiler_params=pltpu.CompilerParams(vmem_limit_bytes=32 * 1024 * 1024),
    )(me, block_table, seq_lens, query_rows, *arrived)
    attended = attended.reshape(sequence_total, attention_head_count * LATENT_RANK)
    return (expert_out, attended)


def solution(mesh):
    return jax.shard_map(
        layer,
        mesh=mesh,
        in_specs=(
            P(("groups", "ep"), None),
            P(("groups", "ep"), None),
            P(),
            P(None, "ep"),
            P(None, "ep"),
            P("ep", None),
            P(("groups", "ep"), None),
            P(("groups", "ep"), None),
            P(("groups", "ep"), None),
            P(("groups", "ep")),
            P(("groups", "ep"), None),
        ),
        out_specs=(P(("groups", "ep"), None), P(("groups", "ep"), None)),
        check_vma=False,
    )
```

```python
import functools

import jax
import jax.numpy as jnp
from jax import lax
from jax.experimental import pallas as pl
from jax.experimental.pallas import tpu as pltpu
from jax.sharding import PartitionSpec as P


LATENT_RANK = 512
ROTARY_WIDTH = 64
BLOCK = 8


route_scale = 2.5
softmax_scale = 192.0 ** (-0.5)


def vmem():
    return pl.BlockSpec(memory_space=pltpu.VMEM)


def smem():
    return pl.BlockSpec(memory_space=pltpu.SMEM)


def in_hbm(value):
    return pltpu.with_memory_space_constraint(value, pltpu.HBM)


def placements(routes_ref, mine, blocks, caps, axis):
    top, tok_rows = routes_ref.shape
    shape = (blocks * caps, 128) if axis == 0 else (tok_rows, blocks * caps)
    row = lax.broadcasted_iota(jnp.int32, shape, axis)
    expert = (row // caps) ^ mine
    slot = row % caps
    count = jnp.zeros(shape, jnp.int32)
    out = []
    for t in range(tok_rows):
        hit = expert == routes_ref[0, t]
        for j in range(1, top):
            hit = hit | (expert == routes_ref[j, t])
        out.append(hit & (count == slot))
        count = count + hit.astype(jnp.int32)
    return out


def pack_kernel(caps, mine_ref, routes_ref, tokens_ref, *out_refs):
    blocks = len(out_refs)
    width = tokens_ref.shape[1]
    placed = placements(routes_ref, mine_ref[0], blocks, caps, 0)
    tokens = tokens_ref[...].astype(jnp.float32)
    rows = jnp.zeros((blocks * caps, width), jnp.float32)
    for t, hit in enumerate(placed):
        rows = rows + jnp.where(hit[:, :1], tokens[t : t + 1, :], 0.0)
    rows = rows.astype(jnp.bfloat16)
    for b in range(blocks):
        out_refs[b][...] = rows[b * caps : (b + 1) * caps, :]


def mix_kernel(caps, mine_ref, routes_ref, tokens_ref, centroids_ref, out_ref):
    top, tok_rows = routes_ref.shape
    experts = centroids_ref.shape[0]
    mine = mine_ref[0]
    scores = jax.nn.sigmoid(
        lax.dot_general(
            tokens_ref[...],
            centroids_ref[...],
            (((1,), (1,)), ((), ())),
            preferred_element_type=jnp.float32,
        )
    )
    expert = lax.broadcasted_iota(jnp.int32, (tok_rows, experts), 1)
    token = lax.broadcasted_iota(jnp.int32, (tok_rows, experts), 0)
    chosen = jnp.zeros((tok_rows, experts), jnp.float32)
    for t in range(tok_rows):
        for j in range(top):
            hit = (token == t) & (expert == routes_ref[j, t])
            chosen = jnp.where(hit, chosen + 1.0, chosen)
    weighted = scores * chosen
    share = route_scale * weighted / jnp.sum(weighted, axis=-1, keepdims=True)
    shape = (tok_rows, experts * caps)
    row = lax.broadcasted_iota(jnp.int32, shape, 1)
    row_expert = (row // caps) ^ mine
    row_share = jnp.zeros(shape, jnp.float32)
    for e in range(experts):
        row_share = jnp.where(row_expert == e, share[:, e : e + 1], row_share)
    placed = placements(routes_ref, mine, experts, caps, 1)
    row_token = lax.broadcasted_iota(jnp.int32, shape, 0)
    mixing = jnp.zeros(shape, jnp.float32)
    for t, hit in enumerate(placed):
        mixing = jnp.where((row_token == t) & hit, row_share, mixing)
    out_ref[...] = mixing


def outgoing_kernel(shards, me_ref, order_ref, pool_ref, *out_refs):
    rows = out_refs[0].shape[0]
    blocks = pool_ref.shape[0]
    total = rows * len(out_refs)
    row = lax.broadcasted_iota(jnp.int32, (total, blocks), 0)
    block = lax.broadcasted_iota(jnp.int32, (total, blocks), 1)
    wanted = jnp.zeros((total, blocks), jnp.int32)
    for i in range(total):
        target = shards * (i % rows // 2) + 2 * (i // rows) + i % 2
        wanted = jnp.where(row == i, order_ref[0, me_ref[0] ^ target], wanted)
    picks = jnp.where(block == wanted, 1.0, 0.0).astype(jnp.bfloat16)
    result = jnp.dot(picks, pool_ref[...], preferred_element_type=jnp.float32)
    for m, out_ref in enumerate(out_refs):
        out_ref[...] = result[m * rows : (m + 1) * rows, :].astype(jnp.bfloat16)


def join_kernel(groups, *refs):
    row_refs, rest = refs[:groups], refs[groups:]
    block_refs, out_refs = rest[: len(rest) // 2], rest[len(rest) // 2 :]
    caps, width = row_refs[0].shape
    for block_ref, out_ref in zip(block_refs, out_refs):
        for b, row_ref in enumerate(row_refs):
            out_ref[b * caps : (b + 1) * caps, :width] = row_ref[...]
        out_ref[:, width:] = block_ref[...]


def leaving_kernel(shift, *refs):
    groups = refs[0].shape[0] // 2
    for b, out_ref in enumerate(refs[len(refs) - groups + 1 :], 1):
        for m, in_ref in enumerate(refs[: len(refs) - groups + 1]):
            out_ref[2 * m : 2 * m + 2, :] = in_ref[2 * b : 2 * b + 2, shift:]


def attention_kernel(
    groups, shards, shift, me_ref, table_ref, lens_ref, queries_ref, *refs
):
    *arrived_refs, out_ref, arrived = refs
    sequences, heads, entries = queries_ref.shape
    pairs = shards // 2
    side = groups * shards
    for a in range(2):
        near_refs = arrived_refs[a * pairs : (a + 1) * pairs]
        far_refs = arrived_refs[2 * pairs + a * (groups - 1) : 2 * pairs + (a + 1) * (groups - 1)]
        for m, near_ref in enumerate(near_refs):
            arrived[a * side + 2 * m : a * side + 2 * m + 2, :] = near_ref[:2, shift:]
        for b, far_ref in enumerate(far_refs, 1):
            start = a * side + b * shards
            arrived[start : start + shards, :] = far_ref[...]
    count = side
    half = count // 2
    row = lax.broadcasted_iota(jnp.int32, (count, 2 * count), 0)
    column = lax.broadcasted_iota(jnp.int32, (count, 2 * count), 1)
    picks = jnp.where(column == 2 * row + row // half, 1.0, 0.0).astype(jnp.bfloat16)
    blocks = jnp.dot(picks, arrived[...], preferred_element_type=jnp.float32).astype(jnp.bfloat16)
    cache = jnp.concatenate(
        [blocks[:, i * entries : (i + 1) * entries] for i in range(BLOCK)], axis=0
    )
    keys = cache.shape[0]
    key = lax.broadcasted_iota(jnp.int32, (1, keys), 1)
    token = key // count
    place = key % count
    source = me_ref[0] ^ (
        place // half + 2 * (place % pairs) + shards * (place % half // pairs)
    )
    per_sequence = count // sequences
    visible = []
    for s in range(sequences):
        position = jnp.full((1, keys), per_sequence * BLOCK, jnp.int32)
        for b in range(per_sequence):
            position = jnp.where(
                source == table_ref[0, s * per_sequence + b], b * BLOCK + token, position
            )
        shown = jnp.where(position < lens_ref[s], 1.0, 0.0)
        visible.append(jnp.broadcast_to(shown, (heads, keys)))
    visible = jnp.concatenate(visible, axis=0) > 0.5
    queries = queries_ref[...].reshape(sequences * heads, entries)
    logits = lax.dot_general(
        queries, cache, (((1,), (1,)), ((), ())), preferred_element_type=jnp.float32
    )
    logits = jnp.where(visible, logits * softmax_scale, -1e30)
    peak = jnp.max(logits, axis=-1, keepdims=True)
    unnormed = jnp.where(visible, jnp.exp(logits - peak), 0.0)
    weights = (unnormed / jnp.sum(unnormed, axis=-1, keepdims=True)).astype(jnp.bfloat16)
    attended = jnp.dot(weights, cache[:, :LATENT_RANK], preferred_element_type=jnp.float32)
    out_ref[...] = attended.astype(jnp.bfloat16).reshape(sequences, heads, LATENT_RANK)


def ffn_kernel(chunks, gate_ref, up_ref, down_ref, *refs):
    *row_refs, keep_ref, send_ref, rows = refs
    width, units = gate_ref.shape
    step = width // chunks
    half = keep_ref.shape[0]
    height = row_refs[0].shape[0]
    for i, row_ref in enumerate(row_refs):
        rows[i * height : (i + 1) * height, :] = row_ref[:, :width]
    gate_sum = jnp.zeros((2 * half, units), jnp.float32)
    up_sum = jnp.zeros((2 * half, units), jnp.float32)
    for i in range(chunks):
        part = pl.ds(i * step, step)
        gate_sum += jnp.dot(rows[:, part], gate_ref[part, :], preferred_element_type=jnp.float32)
        up_sum += jnp.dot(rows[:, part], up_ref[part, :], preferred_element_type=jnp.float32)
    hidden = (gate_sum * jax.nn.sigmoid(gate_sum) * up_sum).astype(jnp.bfloat16)
    for i in range(chunks):
        part = pl.ds(i * step, step)
        result = jnp.dot(hidden, down_ref[:, part], preferred_element_type=jnp.float32)
        result = result.astype(jnp.bfloat16)
        keep_ref[:, part] = result[:half, :]
        send_ref[:, part] = result[half:, :]


def layer(
    tokens,
    routes,
    router_weight,
    w_gate,
    w_up,
    w_down,
    latent_pool,
    send_order,
    block_table,
    seq_lens,
    queries,
):
    device_count = lax.axis_size("ep")
    tok_rows, width = tokens.shape
    experts = router_weight.shape[1]
    top_count = routes.shape[1]
    shard_count = device_count // experts
    capacity = tok_rows * top_count // experts + tok_rows * top_count // (4 * experts)
    me = lax.axis_index("ep").astype(jnp.int32).reshape(1)
    mine = me // shard_count

    def exchange(value, mask):
        return lax.ppermute(value, "ep", [(i, i ^ mask) for i in range(device_count)])

    def kernel(body, **options):
        def call(*operands):
            return pl.pallas_call(body, **options)(*operands)

        return call

    small = pltpu.CompilerParams(vmem_limit_bytes=8 * 1024 * 1024)
    routes = routes.T

    packed = kernel(
        functools.partial(pack_kernel, capacity),
        out_shape=[jax.ShapeDtypeStruct((capacity, width), jnp.bfloat16)] * experts,
        in_specs=[smem(), smem(), vmem()],
        out_specs=[vmem()] * experts,
        compiler_params=small,
    )(mine, in_hbm(routes), in_hbm(tokens))
    crossed = [exchange(packed[b], b * shard_count) for b in range(1, experts)]
    slots = experts * capacity
    assert capacity == 2

    compressed_width = LATENT_RANK + ROTARY_WIDTH
    block_width = latent_pool.shape[1]
    pairs = shard_count // 2
    outgoing = kernel(
        functools.partial(outgoing_kernel, shard_count),
        out_shape=[jax.ShapeDtypeStruct((2 * experts, block_width), jnp.bfloat16)] * pairs,
        in_specs=[smem(), smem(), vmem()],
        out_specs=[vmem()] * pairs,
        compiler_params=small,
    )(me, in_hbm(send_order), in_hbm(latent_pool))
    joined = kernel(
        functools.partial(join_kernel, experts),
        cost_estimate=pl.CostEstimate(
            flops=8 * 10**9, bytes_accessed=8 * 10**7, transcendentals=0
        ),
        out_shape=[jax.ShapeDtypeStruct((slots, width + block_width), jnp.bfloat16)] * pairs,
        in_specs=[vmem()] * (experts + pairs),
        out_specs=[vmem()] * pairs,
        compiler_params=small,
    )(packed[0], *crossed, *outgoing)
    near = [joined[0]] + [exchange(joined[m], 2 * m) for m in range(1, pairs)]
    far = [exchange(piece, 1) for piece in near]
    leaving = kernel(
        functools.partial(leaving_kernel, width),
        out_shape=[jax.ShapeDtypeStruct((shard_count, block_width), jnp.bfloat16)]
        * (experts - 1),
        in_specs=[vmem()] * pairs,
        out_specs=[vmem()] * (experts - 1),
        compiler_params=small,
    )(*near)
    entered = [exchange(leaving[b - 1], b * shard_count) for b in range(1, experts)]
    arrived = near + far + entered + [exchange(piece, 1) for piece in entered]

    half = slots * shard_count // 2
    units = w_gate.shape[1]
    chunks = 7
    keep, send = kernel(
        functools.partial(ffn_kernel, chunks),
        out_shape=[jax.ShapeDtypeStruct((half, width), jnp.bfloat16)] * 2,
        in_specs=[vmem()] * (3 + shard_count),
        out_specs=[vmem(), vmem()],
        scratch_shapes=[pltpu.VMEM((2 * half, width), jnp.bfloat16)],
        compiler_params=pltpu.CompilerParams(vmem_limit_bytes=16 * 1024 * 1024),
        cost_estimate=pl.CostEstimate(
            flops=12 * half * width * units, bytes_accessed=6 * width * units, transcendentals=0
        ),
    )(w_gate, w_up, w_down, *near, *far)

    paired = keep.astype(jnp.float32) + exchange(send, 1).astype(jnp.float32)
    paired = paired.reshape(shard_count // 2, slots, width)
    total = paired[0]
    for k in range(1, shard_count // 2):
        total = total + exchange(paired[k].astype(jnp.bfloat16), 2 * k).astype(jnp.float32)
    total = total.reshape(experts, capacity, width)
    summed = [total[0]] + [
        exchange(total[b].astype(jnp.bfloat16), b * shard_count).astype(jnp.float32)
        for b in range(1, experts)
    ]
    mixing = kernel(
        functools.partial(mix_kernel, capacity),
        out_shape=jax.ShapeDtypeStruct((tok_rows, slots), jnp.float32),
        in_specs=[smem(), smem(), vmem(), vmem()],
        out_specs=vmem(),
        compiler_params=small,
    )(mine, in_hbm(routes), in_hbm(tokens), in_hbm(router_weight.T))
    expert_out = jnp.zeros((tok_rows, width), jnp.float32)
    for b in range(experts):
        for c in range(capacity):
            r = b * capacity + c
            expert_out = expert_out + mixing[:, r : r + 1] * summed[b][c : c + 1, :]
    expert_out = expert_out.astype(jnp.bfloat16)

    sequence_total = seq_lens.shape[0]
    attention_head_count = queries.shape[1] // compressed_width
    query_rows = queries.reshape(sequence_total, attention_head_count, compressed_width)
    attended = kernel(
        functools.partial(attention_kernel, experts, shard_count, width),
        out_shape=jax.ShapeDtypeStruct(
            (sequence_total, attention_head_count, LATENT_RANK), jnp.bfloat16
        ),
        in_specs=[smem()] * 3 + [vmem()] * (1 + len(arrived)),
        out_specs=vmem(),
        scratch_shapes=[pltpu.VMEM((2 * device_count, block_width), jnp.bfloat16)],
        compiler_params=pltpu.CompilerParams(vmem_limit_bytes=32 * 1024 * 1024),
    )(me, block_table, seq_lens, query_rows, *arrived)
    attended = attended.reshape(sequence_total, attention_head_count * LATENT_RANK)
    return (expert_out, attended)


def solution(mesh):
    return jax.shard_map(
        layer,
        mesh=mesh,
        in_specs=(
            P(("groups", "ep"), None),
            P(("groups", "ep"), None),
            P(),
            P(None, "ep"),
            P(None, "ep"),
            P("ep", None),
            P(("groups", "ep"), None),
            P(("groups", "ep"), None),
            P(("groups", "ep"), None),
            P(("groups", "ep")),
            P(("groups", "ep"), None),
        ),
        out_specs=(P(("groups", "ep"), None), P(("groups", "ep"), None)),
        check_vma=False,
    )
```

```python
import functools

import jax
import jax.numpy as jnp
from jax import lax
from jax.experimental import pallas as pl
from jax.experimental.pallas import tpu as pltpu
from jax.sharding import PartitionSpec as P


LATENT_RANK = 512
ROTARY_WIDTH = 64
BLOCK = 8


route_scale = 2.5
softmax_scale = 192.0 ** (-0.5)


def vmem():
    return pl.BlockSpec(memory_space=pltpu.VMEM)


def smem():
    return pl.BlockSpec(memory_space=pltpu.SMEM)


def in_hbm(value):
    return pltpu.with_memory_space_constraint(value, pltpu.HBM)


def placements(routes_ref, mine, blocks, caps, axis):
    top, tok_rows = routes_ref.shape
    shape = (blocks * caps, 128) if axis == 0 else (tok_rows, blocks * caps)
    row = lax.broadcasted_iota(jnp.int32, shape, axis)
    expert = (row // caps) ^ mine
    slot = row % caps
    count = jnp.zeros(shape, jnp.int32)
    out = []
    for t in range(tok_rows):
        hit = expert == routes_ref[0, t]
        for j in range(1, top):
            hit = hit | (expert == routes_ref[j, t])
        out.append(hit & (count == slot))
        count = count + hit.astype(jnp.int32)
    return out


def pack_kernel(caps, mine_ref, routes_ref, tokens_ref, *out_refs):
    blocks = len(out_refs)
    width = tokens_ref.shape[1]
    placed = placements(routes_ref, mine_ref[0], blocks, caps, 0)
    tokens = tokens_ref[...].astype(jnp.float32)
    rows = jnp.zeros((blocks * caps, width), jnp.float32)
    for t, hit in enumerate(placed):
        rows = rows + jnp.where(hit[:, :1], tokens[t : t + 1, :], 0.0)
    rows = rows.astype(jnp.bfloat16)
    for b in range(blocks):
        out_refs[b][...] = rows[b * caps : (b + 1) * caps, :]


def mix_kernel(caps, mine_ref, routes_ref, tokens_ref, centroids_ref, out_ref):
    top, tok_rows = routes_ref.shape
    experts = centroids_ref.shape[0]
    mine = mine_ref[0]
    scores = jax.nn.sigmoid(
        lax.dot_general(
            tokens_ref[...],
            centroids_ref[...],
            (((1,), (1,)), ((), ())),
            preferred_element_type=jnp.float32,
        )
    )
    expert = lax.broadcasted_iota(jnp.int32, (tok_rows, experts), 1)
    token = lax.broadcasted_iota(jnp.int32, (tok_rows, experts), 0)
    chosen = jnp.zeros((tok_rows, experts), jnp.float32)
    for t in range(tok_rows):
        for j in range(top):
            hit = (token == t) & (expert == routes_ref[j, t])
            chosen = jnp.where(hit, chosen + 1.0, chosen)
    weighted = scores * chosen
    share = route_scale * weighted / jnp.sum(weighted, axis=-1, keepdims=True)
    shape = (tok_rows, experts * caps)
    row = lax.broadcasted_iota(jnp.int32, shape, 1)
    row_expert = (row // caps) ^ mine
    row_share = jnp.zeros(shape, jnp.float32)
    for e in range(experts):
        row_share = jnp.where(row_expert == e, share[:, e : e + 1], row_share)
    placed = placements(routes_ref, mine, experts, caps, 1)
    row_token = lax.broadcasted_iota(jnp.int32, shape, 0)
    mixing = jnp.zeros(shape, jnp.float32)
    for t, hit in enumerate(placed):
        mixing = jnp.where((row_token == t) & hit, row_share, mixing)
    out_ref[...] = mixing


def outgoing_kernel(shards, me_ref, order_ref, pool_ref, *out_refs):
    rows = out_refs[0].shape[0]
    blocks = pool_ref.shape[0]
    total = rows * len(out_refs)
    row = lax.broadcasted_iota(jnp.int32, (total, blocks), 0)
    block = lax.broadcasted_iota(jnp.int32, (total, blocks), 1)
    wanted = jnp.zeros((total, blocks), jnp.int32)
    for i in range(total):
        target = shards * (i % rows // 2) + 2 * (i // rows) + i % 2
        wanted = jnp.where(row == i, order_ref[0, me_ref[0] ^ target], wanted)
    picks = jnp.where(block == wanted, 1.0, 0.0).astype(jnp.bfloat16)
    result = jnp.dot(picks, pool_ref[...], preferred_element_type=jnp.float32)
    for m, out_ref in enumerate(out_refs):
        out_ref[...] = result[m * rows : (m + 1) * rows, :].astype(jnp.bfloat16)


def entry_kernel(
    caps, shards, mine_ref, routes_ref, me_ref, order_ref, tokens_ref, pool_ref, *out_refs
):
    groups = len(out_refs) - shards // 2
    pack_kernel(caps, mine_ref, routes_ref, tokens_ref, *out_refs[:groups])
    outgoing_kernel(shards, me_ref, order_ref, pool_ref, *out_refs[groups:])


def join_kernel(*refs):
    *in_refs, out_ref = refs
    rows = in_refs[0].shape[0]
    for i, in_ref in enumerate(in_refs):
        out_ref[i * rows : (i + 1) * rows, :] = in_ref[...]


def sorting_kernel(*refs):
    groups = refs[0].shape[0] // 2
    in_refs, out_refs = refs[:-groups], refs[-groups:]
    for b, out_ref in enumerate(out_refs):
        for m, in_ref in enumerate(in_refs):
            out_ref[2 * m : 2 * m + 2, :] = in_ref[2 * b : 2 * b + 2, :]


def attention_kernel(groups, shards, me_ref, table_ref, lens_ref, queries_ref, *refs):
    *arrived_refs, out_ref, arrived = refs
    sequences, heads, entries = queries_ref.shape
    pairs = shards // 2
    side = groups * shards
    for i, arrived_ref in enumerate(arrived_refs):
        arrived[i * shards : (i + 1) * shards, :] = arrived_ref[...]
    count = side
    half = count // 2
    row = lax.broadcasted_iota(jnp.int32, (count, 2 * count), 0)
    column = lax.broadcasted_iota(jnp.int32, (count, 2 * count), 1)
    picks = jnp.where(column == 2 * row + row // half, 1.0, 0.0).astype(jnp.bfloat16)
    blocks = jnp.dot(picks, arrived[...], preferred_element_type=jnp.float32).astype(jnp.bfloat16)
    cache = jnp.concatenate(
        [blocks[:, i * entries : (i + 1) * entries] for i in range(BLOCK)], axis=0
    )
    keys = cache.shape[0]
    key = lax.broadcasted_iota(jnp.int32, (1, keys), 1)
    token = key // count
    place = key % count
    source = me_ref[0] ^ (
        place // half + 2 * (place % pairs) + shards * (place % half // pairs)
    )
    per_sequence = count // sequences
    visible = []
    for s in range(sequences):
        position = jnp.full((1, keys), per_sequence * BLOCK, jnp.int32)
        for b in range(per_sequence):
            position = jnp.where(
                source == table_ref[0, s * per_sequence + b], b * BLOCK + token, position
            )
        shown = jnp.where(position < lens_ref[s], 1.0, 0.0)
        visible.append(jnp.broadcast_to(shown, (heads, keys)))
    visible = jnp.concatenate(visible, axis=0) > 0.5
    queries = queries_ref[...].reshape(sequences * heads, entries)
    logits = lax.dot_general(
        queries, cache, (((1,), (1,)), ((), ())), preferred_element_type=jnp.float32
    )
    logits = jnp.where(visible, logits * softmax_scale, -1e30)
    peak = jnp.max(logits, axis=-1, keepdims=True)
    unnormed = jnp.where(visible, jnp.exp(logits - peak), 0.0)
    weights = (unnormed / jnp.sum(unnormed, axis=-1, keepdims=True)).astype(jnp.bfloat16)
    attended = jnp.dot(weights, cache[:, :LATENT_RANK], preferred_element_type=jnp.float32)
    out_ref[...] = attended.astype(jnp.bfloat16).reshape(sequences, heads, LATENT_RANK)


def ffn_kernel(chunks, gate_ref, up_ref, down_ref, *refs):
    *row_refs, keep_ref, send_ref, rows = refs
    width, units = gate_ref.shape
    step = width // chunks
    half = keep_ref.shape[0]
    height = row_refs[0].shape[0]
    for i, row_ref in enumerate(row_refs):
        rows[i * height : (i + 1) * height, :] = row_ref[:, :width]
    gate_sum = jnp.zeros((2 * half, units), jnp.float32)
    up_sum = jnp.zeros((2 * half, units), jnp.float32)
    for i in range(chunks):
        part = pl.ds(i * step, step)
        gate_sum += jnp.dot(rows[:, part], gate_ref[part, :], preferred_element_type=jnp.float32)
        up_sum += jnp.dot(rows[:, part], up_ref[part, :], preferred_element_type=jnp.float32)
    hidden = (gate_sum * jax.nn.sigmoid(gate_sum) * up_sum).astype(jnp.bfloat16)
    for i in range(chunks):
        part = pl.ds(i * step, step)
        result = jnp.dot(hidden, down_ref[:, part], preferred_element_type=jnp.float32)
        result = result.astype(jnp.bfloat16)
        keep_ref[:, part] = result[:half, :]
        send_ref[:, part] = result[half:, :]


def layer(
    tokens,
    routes,
    router_weight,
    w_gate,
    w_up,
    w_down,
    latent_pool,
    send_order,
    block_table,
    seq_lens,
    queries,
):
    device_count = lax.axis_size("ep")
    tok_rows, width = tokens.shape
    experts = router_weight.shape[1]
    top_count = routes.shape[1]
    shard_count = device_count // experts
    capacity = tok_rows * top_count // experts + tok_rows * top_count // (4 * experts)
    me = lax.axis_index("ep").astype(jnp.int32).reshape(1)
    mine = me // shard_count

    def exchange(value, mask):
        return lax.ppermute(value, "ep", [(i, i ^ mask) for i in range(device_count)])

    def kernel(body, **options):
        def call(*operands):
            return pl.pallas_call(body, **options)(*operands)

        return call

    small = pltpu.CompilerParams(vmem_limit_bytes=8 * 1024 * 1024)
    routes = routes.T

    block_width = latent_pool.shape[1]
    pairs = shard_count // 2
    entry = kernel(
        functools.partial(entry_kernel, capacity, shard_count),
        out_shape=[jax.ShapeDtypeStruct((capacity, width), jnp.bfloat16)] * experts
        + [jax.ShapeDtypeStruct((2 * experts, block_width), jnp.bfloat16)] * pairs,
        in_specs=[smem()] * 4 + [vmem()] * 2,
        out_specs=[vmem()] * (experts + pairs),
        compiler_params=small,
    )(
        mine,
        in_hbm(routes),
        me,
        in_hbm(send_order),
        in_hbm(tokens),
        in_hbm(latent_pool),
    )
    packed, outgoing = entry[:experts], entry[experts:]
    crossed = [exchange(packed[b], b * shard_count) for b in range(1, experts)]
    slots = experts * capacity
    assert capacity == 2

    compressed_width = LATENT_RANK + ROTARY_WIDTH
    spread = [outgoing[0]] + [exchange(outgoing[m], 2 * m) for m in range(1, pairs)]
    staying, *leaving = kernel(
        sorting_kernel,
        out_shape=[jax.ShapeDtypeStruct((shard_count, block_width), jnp.bfloat16)] * experts,
        in_specs=[vmem()] * pairs,
        out_specs=[vmem()] * experts,
        compiler_params=small,
    )(*spread)
    entered = [exchange(piece, b * shard_count) for b, piece in enumerate(leaving, 1)]
    arrived = [staying] + entered
    arrived = arrived + [exchange(piece, 1) for piece in arrived]

    rows = kernel(
        join_kernel,
        cost_estimate=pl.CostEstimate(
            flops=8 * 10**9, bytes_accessed=8 * 10**7, transcendentals=0
        ),
        out_shape=jax.ShapeDtypeStruct((slots, width), jnp.bfloat16),
        in_specs=[vmem()] * experts,
        out_specs=vmem(),
        compiler_params=small,
    )(packed[0], *crossed)
    near = [rows] + [exchange(rows, 2 * m) for m in range(1, pairs)]
    far = [exchange(piece, 1) for piece in near]

    half = slots * shard_count // 2
    units = w_gate.shape[1]
    chunks = 7
    keep, send = kernel(
        functools.partial(ffn_kernel, chunks),
        out_shape=[jax.ShapeDtypeStruct((half, width), jnp.bfloat16)] * 2,
        in_specs=[vmem()] * (3 + shard_count),
        out_specs=[vmem(), vmem()],
        scratch_shapes=[pltpu.VMEM((2 * half, width), jnp.bfloat16)],
        compiler_params=pltpu.CompilerParams(vmem_limit_bytes=16 * 1024 * 1024),
        cost_estimate=pl.CostEstimate(
            flops=12 * half * width * units, bytes_accessed=6 * width * units, transcendentals=0
        ),
    )(w_gate, w_up, w_down, *near, *far)

    paired = keep.astype(jnp.float32) + exchange(send, 1).astype(jnp.float32)
    paired = paired.reshape(shard_count // 2, slots, width)
    total = paired[0]
    for k in range(1, shard_count // 2):
        total = total + exchange(paired[k].astype(jnp.bfloat16), 2 * k).astype(jnp.float32)
    total = total.reshape(experts, capacity, width)
    summed = [total[0]] + [
        exchange(total[b].astype(jnp.bfloat16), b * shard_count).astype(jnp.float32)
        for b in range(1, experts)
    ]
    mixing = kernel(
        functools.partial(mix_kernel, capacity),
        out_shape=jax.ShapeDtypeStruct((tok_rows, slots), jnp.float32),
        in_specs=[smem(), smem(), vmem(), vmem()],
        out_specs=vmem(),
        compiler_params=small,
    )(mine, in_hbm(routes), in_hbm(tokens), in_hbm(router_weight.T))
    expert_out = jnp.zeros((tok_rows, width), jnp.float32)
    for b in range(experts):
        for c in range(capacity):
            r = b * capacity + c
            expert_out = expert_out + mixing[:, r : r + 1] * summed[b][c : c + 1, :]
    expert_out = expert_out.astype(jnp.bfloat16)

    sequence_total = seq_lens.shape[0]
    attention_head_count = queries.shape[1] // compressed_width
    query_rows = queries.reshape(sequence_total, attention_head_count, compressed_width)
    attended = kernel(
        functools.partial(attention_kernel, experts, shard_count),
        out_shape=jax.ShapeDtypeStruct(
            (sequence_total, attention_head_count, LATENT_RANK), jnp.bfloat16
        ),
        in_specs=[smem()] * 3 + [vmem()] * (1 + len(arrived)),
        out_specs=vmem(),
        scratch_shapes=[pltpu.VMEM((2 * device_count, block_width), jnp.bfloat16)],
        compiler_params=pltpu.CompilerParams(vmem_limit_bytes=32 * 1024 * 1024),
    )(me, block_table, seq_lens, query_rows, *arrived)
    attended = attended.reshape(sequence_total, attention_head_count * LATENT_RANK)
    return (expert_out, attended)


def solution(mesh):
    return jax.shard_map(
        layer,
        mesh=mesh,
        in_specs=(
            P(("groups", "ep"), None),
            P(("groups", "ep"), None),
            P(),
            P(None, "ep"),
            P(None, "ep"),
            P("ep", None),
            P(("groups", "ep"), None),
            P(("groups", "ep"), None),
            P(("groups", "ep"), None),
            P(("groups", "ep")),
            P(("groups", "ep"), None),
        ),
        out_specs=(P(("groups", "ep"), None), P(("groups", "ep"), None)),
        check_vma=False,
    )
```

```python
import functools

import jax
import jax.numpy as jnp
from jax import lax
from jax.experimental import pallas as pl
from jax.experimental.pallas import tpu as pltpu
from jax.sharding import PartitionSpec as P


LATENT_RANK = 512
ROTARY_WIDTH = 64
BLOCK = 8


route_scale = 2.5
softmax_scale = 192.0 ** (-0.5)


def vmem():
    return pl.BlockSpec(memory_space=pltpu.VMEM)


def smem():
    return pl.BlockSpec(memory_space=pltpu.SMEM)


def in_hbm(value):
    return pltpu.with_memory_space_constraint(value, pltpu.HBM)


def placements(routes_ref, mine, blocks, caps, axis):
    top, tok_rows = routes_ref.shape
    shape = (blocks * caps, 128) if axis == 0 else (tok_rows, blocks * caps)
    row = lax.broadcasted_iota(jnp.int32, shape, axis)
    expert = (row // caps) ^ mine
    slot = row % caps
    count = jnp.zeros(shape, jnp.int32)
    out = []
    for t in range(tok_rows):
        hit = expert == routes_ref[0, t]
        for j in range(1, top):
            hit = hit | (expert == routes_ref[j, t])
        out.append(hit & (count == slot))
        count = count + hit.astype(jnp.int32)
    return out


def pack_kernel(caps, mine_ref, routes_ref, tokens_ref, *out_refs):
    blocks = len(out_refs)
    width = tokens_ref.shape[1]
    placed = placements(routes_ref, mine_ref[0], blocks, caps, 0)
    tokens = tokens_ref[...].astype(jnp.float32)
    rows = jnp.zeros((blocks * caps, width), jnp.float32)
    for t, hit in enumerate(placed):
        rows = rows + jnp.where(hit[:, :1], tokens[t : t + 1, :], 0.0)
    rows = rows.astype(jnp.bfloat16)
    for b in range(blocks):
        out_refs[b][...] = rows[b * caps : (b + 1) * caps, :]


def mix_kernel(caps, mine_ref, routes_ref, tokens_ref, centroids_ref, out_ref):
    top, tok_rows = routes_ref.shape
    experts = centroids_ref.shape[0]
    mine = mine_ref[0]
    scores = jax.nn.sigmoid(
        lax.dot_general(
            tokens_ref[...],
            centroids_ref[...],
            (((1,), (1,)), ((), ())),
            preferred_element_type=jnp.float32,
        )
    )
    expert = lax.broadcasted_iota(jnp.int32, (tok_rows, experts), 1)
    token = lax.broadcasted_iota(jnp.int32, (tok_rows, experts), 0)
    chosen = jnp.zeros((tok_rows, experts), jnp.float32)
    for t in range(tok_rows):
        for j in range(top):
            hit = (token == t) & (expert == routes_ref[j, t])
            chosen = jnp.where(hit, chosen + 1.0, chosen)
    weighted = scores * chosen
    share = route_scale * weighted / jnp.sum(weighted, axis=-1, keepdims=True)
    shape = (tok_rows, experts * caps)
    row = lax.broadcasted_iota(jnp.int32, shape, 1)
    row_expert = (row // caps) ^ mine
    row_share = jnp.zeros(shape, jnp.float32)
    for e in range(experts):
        row_share = jnp.where(row_expert == e, share[:, e : e + 1], row_share)
    placed = placements(routes_ref, mine, experts, caps, 1)
    row_token = lax.broadcasted_iota(jnp.int32, shape, 0)
    mixing = jnp.zeros(shape, jnp.float32)
    for t, hit in enumerate(placed):
        mixing = jnp.where((row_token == t) & hit, row_share, mixing)
    out_ref[...] = mixing


def outgoing_kernel(shards, me_ref, order_ref, pool_ref, *out_refs):
    rows = out_refs[0].shape[0]
    blocks = pool_ref.shape[0]
    total = rows * len(out_refs)
    row = lax.broadcasted_iota(jnp.int32, (total, blocks), 0)
    block = lax.broadcasted_iota(jnp.int32, (total, blocks), 1)
    wanted = jnp.zeros((total, blocks), jnp.int32)
    for i in range(total):
        m, b, r = i // rows, i % rows // 2, i % 2
        target = shards * b + 2 * m + (r ^ (b > 0) ^ (m > 0))
        wanted = jnp.where(row == i, order_ref[0, me_ref[0] ^ target], wanted)
    picks = jnp.where(block == wanted, 1.0, 0.0).astype(jnp.bfloat16)
    result = jnp.dot(picks, pool_ref[...], preferred_element_type=jnp.float32)
    for m, out_ref in enumerate(out_refs):
        out_ref[...] = result[m * rows : (m + 1) * rows, :].astype(jnp.bfloat16)


def entry_kernel(
    caps, shards, mine_ref, routes_ref, me_ref, order_ref, tokens_ref, pool_ref, *out_refs
):
    groups = len(out_refs) - shards // 2
    pack_kernel(caps, mine_ref, routes_ref, tokens_ref, *out_refs[:groups])
    outgoing_kernel(shards, me_ref, order_ref, pool_ref, *out_refs[groups:])


def join_kernel(*refs):
    *in_refs, out_ref = refs
    rows = in_refs[0].shape[0]
    for i, in_ref in enumerate(in_refs):
        out_ref[i * rows : (i + 1) * rows, :] = in_ref[...]


def sorting_kernel(*refs):
    groups = refs[0].shape[0] // 2
    in_refs, out_refs = refs[:-groups], refs[-groups:]
    for b, out_ref in enumerate(out_refs):
        for m, in_ref in enumerate(in_refs):
            out_ref[2 * m : 2 * m + 2, :] = in_ref[2 * b : 2 * b + 2, :]


def attention_kernel(groups, shards, me_ref, table_ref, lens_ref, queries_ref, *refs):
    *arrived_refs, out_ref, arrived = refs
    sequences, heads, entries = queries_ref.shape
    pairs = shards // 2
    for i, arrived_ref in enumerate(arrived_refs):
        arrived[i * shards : (i + 1) * shards, :] = arrived_ref[...]
    count = groups * shards
    half = count // 2
    row = lax.broadcasted_iota(jnp.int32, (count, 2 * count), 0)
    column = lax.broadcasted_iota(jnp.int32, (count, 2 * count), 1)
    picks = jnp.where(column == 2 * row + row // half, 1.0, 0.0).astype(jnp.bfloat16)
    blocks = jnp.dot(picks, arrived[...], preferred_element_type=jnp.float32).astype(jnp.bfloat16)
    cache = jnp.concatenate(
        [blocks[:, i * entries : (i + 1) * entries] for i in range(BLOCK)], axis=0
    )
    keys = cache.shape[0]
    key = lax.broadcasted_iota(jnp.int32, (1, keys), 1)
    token = key // count
    place = key % count
    side = place // half
    group = place % half // pairs
    pair = place % pairs
    turns = side + jnp.where(group > 0, 1, 0) + jnp.where(pair > 0, 1, 0)
    source = me_ref[0] ^ (turns % 2 + 2 * pair + shards * group)
    per_sequence = count // sequences
    visible = []
    for s in range(sequences):
        position = jnp.full((1, keys), per_sequence * BLOCK, jnp.int32)
        for b in range(per_sequence):
            position = jnp.where(
                source == table_ref[0, s * per_sequence + b], b * BLOCK + token, position
            )
        shown = jnp.where(position < lens_ref[s], 1.0, 0.0)
        visible.append(jnp.broadcast_to(shown, (heads, keys)))
    visible = jnp.concatenate(visible, axis=0) > 0.5
    queries = queries_ref[...].reshape(sequences * heads, entries)
    logits = lax.dot_general(
        queries, cache, (((1,), (1,)), ((), ())), preferred_element_type=jnp.float32
    )
    logits = jnp.where(visible, logits * softmax_scale, -1e30)
    peak = jnp.max(logits, axis=-1, keepdims=True)
    unnormed = jnp.where(visible, jnp.exp(logits - peak), 0.0)
    weights = (unnormed / jnp.sum(unnormed, axis=-1, keepdims=True)).astype(jnp.bfloat16)
    attended = jnp.dot(weights, cache[:, :LATENT_RANK], preferred_element_type=jnp.float32)
    out_ref[...] = attended.astype(jnp.bfloat16).reshape(sequences, heads, LATENT_RANK)


def ffn_kernel(chunks, gate_ref, up_ref, down_ref, *refs):
    *row_refs, keep_ref, send_ref, rows = refs
    width, units = gate_ref.shape
    step = width // chunks
    half = keep_ref.shape[0]
    height = row_refs[0].shape[0]
    for i, row_ref in enumerate(row_refs):
        rows[i * height : (i + 1) * height, :] = row_ref[:, :width]
    gate_sum = jnp.zeros((2 * half, units), jnp.float32)
    up_sum = jnp.zeros((2 * half, units), jnp.float32)
    for i in range(chunks):
        part = pl.ds(i * step, step)
        gate_sum += jnp.dot(rows[:, part], gate_ref[part, :], preferred_element_type=jnp.float32)
        up_sum += jnp.dot(rows[:, part], up_ref[part, :], preferred_element_type=jnp.float32)
    hidden = (gate_sum * jax.nn.sigmoid(gate_sum) * up_sum).astype(jnp.bfloat16)
    for i in range(chunks):
        part = pl.ds(i * step, step)
        result = jnp.dot(hidden, down_ref[:, part], preferred_element_type=jnp.float32)
        result = result.astype(jnp.bfloat16)
        keep_ref[:, part] = result[:half, :]
        send_ref[:, part] = result[half:, :]


def layer(
    tokens,
    routes,
    router_weight,
    w_gate,
    w_up,
    w_down,
    latent_pool,
    send_order,
    block_table,
    seq_lens,
    queries,
):
    device_count = lax.axis_size("ep")
    tok_rows, width = tokens.shape
    experts = router_weight.shape[1]
    top_count = routes.shape[1]
    shard_count = device_count // experts
    capacity = tok_rows * top_count // experts + tok_rows * top_count // (4 * experts)
    me = lax.axis_index("ep").astype(jnp.int32).reshape(1)
    mine = me // shard_count

    def exchange(value, mask):
        return lax.ppermute(value, "ep", [(i, i ^ mask) for i in range(device_count)])

    def kernel(body, **options):
        def call(*operands):
            return pl.pallas_call(body, **options)(*operands)

        return call

    small = pltpu.CompilerParams(vmem_limit_bytes=8 * 1024 * 1024)
    routes = routes.T

    block_width = latent_pool.shape[1]
    pairs = shard_count // 2
    entry = kernel(
        functools.partial(entry_kernel, capacity, shard_count),
        out_shape=[jax.ShapeDtypeStruct((capacity, width), jnp.bfloat16)] * experts
        + [jax.ShapeDtypeStruct((2 * experts, block_width), jnp.bfloat16)] * pairs,
        in_specs=[smem()] * 4 + [vmem()] * 2,
        out_specs=[vmem()] * (experts + pairs),
        compiler_params=small,
    )(
        mine,
        in_hbm(routes),
        me,
        in_hbm(send_order),
        in_hbm(tokens),
        in_hbm(latent_pool),
    )
    packed, outgoing = entry[:experts], entry[experts:]
    crossed = [exchange(packed[b], b * shard_count + 1) for b in range(1, experts)]
    slots = experts * capacity
    assert capacity == 2

    compressed_width = LATENT_RANK + ROTARY_WIDTH
    spread = [outgoing[0]] + [exchange(outgoing[m], 2 * m + 1) for m in range(1, pairs)]
    staying, *leaving = kernel(
        sorting_kernel,
        out_shape=[jax.ShapeDtypeStruct((shard_count, block_width), jnp.bfloat16)] * experts,
        in_specs=[vmem()] * pairs,
        out_specs=[vmem()] * experts,
        compiler_params=small,
    )(*spread)
    entered = [exchange(piece, b * shard_count + 1) for b, piece in enumerate(leaving, 1)]
    arrived = [staying] + entered
    arrived = arrived + [exchange(piece, 1) for piece in arrived]

    rows = kernel(
        join_kernel,
        cost_estimate=pl.CostEstimate(
            flops=8 * 10**9, bytes_accessed=8 * 10**7, transcendentals=0
        ),
        out_shape=jax.ShapeDtypeStruct((slots, width), jnp.bfloat16),
        in_specs=[vmem()] * experts,
        out_specs=vmem(),
        compiler_params=small,
    )(packed[0], *crossed)
    near = [rows] + [exchange(rows, 2 * m + 1) for m in range(1, pairs)]
    far = [exchange(piece, 1) for piece in near]

    half = slots * shard_count // 2
    units = w_gate.shape[1]
    chunks = 7
    keep, send = kernel(
        functools.partial(ffn_kernel, chunks),
        out_shape=[jax.ShapeDtypeStruct((half, width), jnp.bfloat16)] * 2,
        in_specs=[vmem()] * (3 + shard_count),
        out_specs=[vmem(), vmem()],
        scratch_shapes=[pltpu.VMEM((2 * half, width), jnp.bfloat16)],
        compiler_params=pltpu.CompilerParams(vmem_limit_bytes=16 * 1024 * 1024),
        cost_estimate=pl.CostEstimate(
            flops=12 * half * width * units, bytes_accessed=6 * width * units, transcendentals=0
        ),
    )(w_gate, w_up, w_down, *near, *far)

    sequence_total = seq_lens.shape[0]
    attention_head_count = queries.shape[1] // compressed_width
    query_rows = queries.reshape(sequence_total, attention_head_count, compressed_width)
    attended = kernel(
        functools.partial(attention_kernel, experts, shard_count),
        out_shape=jax.ShapeDtypeStruct(
            (sequence_total, attention_head_count, LATENT_RANK), jnp.bfloat16
        ),
        in_specs=[smem()] * 3 + [vmem()] * (1 + len(arrived)),
        out_specs=vmem(),
        scratch_shapes=[pltpu.VMEM((2 * device_count, block_width), jnp.bfloat16)],
        compiler_params=pltpu.CompilerParams(vmem_limit_bytes=32 * 1024 * 1024),
    )(me, block_table, seq_lens, query_rows, *arrived)
    paired = keep.astype(jnp.float32) + exchange(send, 1).astype(jnp.float32)
    paired = paired.reshape(shard_count // 2, slots, width)
    total = paired[0]
    for k in range(1, shard_count // 2):
        total = total + exchange(paired[k].astype(jnp.bfloat16), 2 * k + 1).astype(jnp.float32)
    total, attended = lax.optimization_barrier((total, attended))
    attended = attended.reshape(sequence_total, attention_head_count * LATENT_RANK)
    total = total.reshape(experts, capacity, width)
    summed = [total[0]] + [
        exchange(total[b].astype(jnp.bfloat16), b * shard_count + 1).astype(jnp.float32)
        for b in range(1, experts)
    ]
    mixing = kernel(
        functools.partial(mix_kernel, capacity),
        out_shape=jax.ShapeDtypeStruct((tok_rows, slots), jnp.float32),
        in_specs=[smem(), smem(), vmem(), vmem()],
        out_specs=vmem(),
        compiler_params=small,
    )(mine, in_hbm(routes), in_hbm(tokens), in_hbm(router_weight.T))
    expert_out = jnp.zeros((tok_rows, width), jnp.float32)
    for b in range(experts):
        for c in range(capacity):
            r = b * capacity + c
            expert_out = expert_out + mixing[:, r : r + 1] * summed[b][c : c + 1, :]
    expert_out = expert_out.astype(jnp.bfloat16)

    return (expert_out, attended)


def solution(mesh):
    return jax.shard_map(
        layer,
        mesh=mesh,
        in_specs=(
            P(("groups", "ep"), None),
            P(("groups", "ep"), None),
            P(),
            P(None, "ep"),
            P(None, "ep"),
            P("ep", None),
            P(("groups", "ep"), None),
            P(("groups", "ep"), None),
            P(("groups", "ep"), None),
            P(("groups", "ep")),
            P(("groups", "ep"), None),
        ),
        out_specs=(P(("groups", "ep"), None), P(("groups", "ep"), None)),
        check_vma=False,
    )
```
